32 devices in a mesh: groups: 2 (over y), seq: 4 (over z), section: 2 (over x), kv: 2 (over core).
Axes of the slice: x: 2, y: 2, z: 4, core: 2. Of those that a mesh axis runs over, the one named last changes fastest.
Arguments:
- queries: bfloat16 [4, 1024, 2560], P(('groups', 'section'), 'seq', 'kv'), parts along dimension 0, may hold values from -128 to 128
- key_rows: bfloat16 [4, 1024, 512], P(('groups', 'section'), 'seq', 'kv'), parts along dimension 0, may hold values from -4 to 4
- values: bfloat16 [4, 1024, 512], P(('groups', 'section'), 'seq', 'kv'), parts along dimension 0, may hold values from -6 to 6
- lengths: int32 [4, 3], P(('groups', 'section')), parts along dimension 0, may hold values from 1 to 32, 64 in all within a row
- block_order: int32 [4, 4], P(('groups', 'section')), parts along dimension 0, may hold values from 0 to 3, each once within a row
- page_owner: int32 [4, 64, 1], P(('groups', 'section')), parts along dimension 0, may hold values from 0 to 3; in each aligned block of 16 rows (0 to 15, 16 to 31, ..., all dimensions but the last counted through in order) at most 8 rows name the same one
Outputs:
- handed: bfloat16 [4, 1024, 2560], P(('groups', 'section'), 'seq', 'kv'), parts along dimension 0
- cache_keys: bfloat16 [4, 4, 512, 512], P(('groups', 'section'), 'seq', None, 'kv'), parts along dimension 0
- cache_values: bfloat16 [4, 4, 512, 512], P(('groups', 'section'), 'seq', None, 'kv'), parts along dimension 0
The draws below stay inside these ranges and needn't reach their ends.
There are 2 independent parts, one for each index of `groups`. The reference program is written for one: setup_inputs(seed, part) draws one part's arguments, and reference() takes and returns one part's arrays. A program takes and returns all parts, laid end to end along the dimension named above; each array names one. Nothing has to cross between parts.
Inputs may be any that keep to these rules, and one draw needn't show every extreme that they name: `lengths`: lengths sum to 64; the longest request has exactly 32 pages. `block_order`: each row is a permutation of the seq indices. `page_owner`: among the 16 pages of one aligned device block, no owner is named more than 8 times.
All inputs are finite; a program needn't handle non-finite values.
Results may differ from the reference program's by a relative error of at most 0.0038.
Values may be sent and summed in bfloat16 or wider, within the bound.
A program may use at most 64 MiB of HBM per device.

```python
import math
import jax
import jax.numpy as jnp
import numpy as np
from jax import lax

QUERY_HEADS = 20
LOCAL_KV_HEADS = 4
HEAD_SIZE = 128
PAGE_TOKENS = 16
REQS = 3
TOK_DEV = 256
RELAY_SECTIONS = 2
SECTION_TOKENS = 1024
PAGES = 64
DEVICE_PAGES = 16
MOST_PAGES = 32
SOURCE_SLOTS = 8
OWNER_CACHE_ROWS = 512
N_SEQ = 4


def shared_pair(base_key):
    initial_random_key = jax.random.fold_in(base_key, 7101)
    second_key = jax.random.fold_in(base_key, 7102)
    per_head_keys = jnp.clip(jax.random.normal(initial_random_key, (RELAY_SECTIONS, SECTION_TOKENS, LOCAL_KV_HEADS, HEAD_SIZE), jnp.float32), -4.0, 4.0)
    per_head_queries = jnp.clip(jax.random.normal(second_key, (RELAY_SECTIONS, SECTION_TOKENS, QUERY_HEADS, HEAD_SIZE), jnp.float32), -4.0, 4.0)
    return (per_head_queries.reshape(RELAY_SECTIONS, SECTION_TOKENS, QUERY_HEADS * HEAD_SIZE), per_head_keys.reshape(RELAY_SECTIONS, SECTION_TOKENS, LOCAL_KV_HEADS * HEAD_SIZE))


def draw_queries(key, part):
    return shared_pair(key)[0].astype(jnp.bfloat16)


def draw_key_rows(key, part):
    return shared_pair(key)[1].astype(jnp.bfloat16)


def block_levels(stream_key, shape, shards, least, largest):
    def one(dim, blocks):
        steps = jax.random.uniform(jax.random.fold_in(jax.random.fold_in(stream_key, 6), dim), (blocks,), jnp.float32, least / len(shards), largest / len(shards))
        return jnp.repeat(jnp.exp(steps), shape[dim] // blocks).reshape((-1,) + (1,) * (len(shape) - dim - 1))

    factor_of = one(*shards[0])
    for cut in shards[1:]:
        factor_of = factor_of * one(*cut)
    return factor_of


def split_up(amount, total, limit, lean):
    weights = [(1 << 20) // math.isqrt(standing ** lean) + 1 for standing in range(2, amount + 1)]
    surplus, holding = total - limit - (amount - 1), [1] * (amount - 1)
    while surplus > 0:
        movable = [i for i in range(amount - 1) if holding[i] < limit]
        mass, budget = sum([weights[i] for i in movable]), surplus
        for i in movable:
            more = min(limit - holding[i], max(1, budget * weights[i] // mass), surplus)
            holding[i] = holding[i] + more
            surplus = surplus - more
    return np.array([limit] + holding)


def ragged_sizes(key, number_of, total, limit, skew):
    if number_of == 2:
        one = jax.random.randint(key, (), max(1, total - limit), min(limit, total - 1) + 1)
        return jnp.stack([one, total - one])
    tallies = jnp.asarray(split_up(number_of, total, limit, skew), jnp.int32)
    pairs = (number_of - 1) // 2
    source_of, receiver = tallies[1:1 + 2 * pairs:2], tallies[2:2 + 2 * pairs:2]
    margin = jnp.minimum(source_of - 1, limit - receiver)
    passed = jax.random.randint(jax.random.fold_in(key, 1), (pairs,), 0, 1 << 20) % (margin + 1)
    tallies = tallies.at[1:1 + 2 * pairs:2].set(source_of - passed).at[2:2 + 2 * pairs:2].set(receiver + passed)
    return tallies[jax.random.permutation(jax.random.fold_in(key, 2), number_of)]


def shared_out(rng, own, number, rows, count, top, most, skew):
    order = jax.random.permutation(rng, count)
    packed, usual = load_shares(count, rows * top, most, skew, True), load_shares(count, rows * top, most, skew, False)
    places = jnp.arange(count)

    def named(sizes, offset_by):
        used = int((sizes > 0).sum())
        fixed = max(1, used // 4)
        moved = fixed + (places - fixed + offset_by * (used - fixed)) % max(1, count - fixed)
        return jnp.zeros((count,), jnp.int32).at[order[jnp.where(places < fixed, places, moved)]].set(jnp.asarray(sizes, jnp.int32))

    sizes = jnp.where(number % 4 == 0, named(packed, number // 4), named(usual, number - number // 4 - 1))
    mixed = jax.random.permutation(jax.random.fold_in(own, 3), count)
    source_of, taker = mixed[0:count // 2 * 2:2], mixed[1:count // 2 * 2:2]
    margin = jnp.minimum(sizes[source_of] - 1, most - sizes[taker]) // 2
    margin = jnp.where((source_of == order[0]) | (taker == order[0]) | (sizes[taker] == 0), 0, jnp.maximum(margin, 0))
    moved = jax.random.randint(jax.random.fold_in(own, 4), (count // 2,), 0, 1 << 20) % (margin + 1)
    sizes = sizes.at[source_of].add(-moved).at[taker].add(moved)
    labels = jnp.searchsorted(jnp.cumsum(sizes), jnp.arange(rows * top), side="right").astype(jnp.int32)
    listing = labels.reshape(top, rows).T
    listing = listing[jax.random.permutation(jax.random.fold_in(own, 1), rows)]
    offset_by = jax.random.randint(jax.random.fold_in(own, 2), (rows, 1), 0, top)
    return jnp.take_along_axis(listing, (jnp.arange(top)[None, :] + offset_by) % top, axis=1)


def load_shares(number_of, total, limit, skew, full):
    loads = [(1 << 20) // math.isqrt(rank ** skew) + 1 for rank in range(1, number_of + 1)]
    largest = limit if full else min(limit, max(-(-total // number_of), total * loads[0] // sum(loads)))
    least = 1 if total - largest >= number_of - 1 else 0
    given, spare = [largest] + [least] * (number_of - 1), total - largest - least * (number_of - 1)
    while spare > 0:
        free = [i for i in range(1, number_of) if given[i] < largest] or [i for i in range(1, number_of) if given[i] < limit]
        mass, budget = sum([loads[i] for i in free]), spare
        for i in free:
            addition = min(limit - given[i], max(1, budget * loads[i] // mass), spare)
            given[i] = given[i] + addition
            spare = spare - addition
    return np.array(given)


def normal_values(stream_key, shape, width, most, cuts=(), kind=jnp.bfloat16):
    level = block_levels(stream_key, shape, cuts, -0.22, 0.18) if cuts else 1.0
    array = jax.random.normal(stream_key, shape, jnp.float32) * width * level
    return jnp.minimum(jnp.maximum(array, -most), most).astype(kind)


def setup_inputs(seed: int = 0, part: int = 0) -> dict:
    key_list = jax.random.split(jax.random.key(seed), 7)
    own_keys = jax.random.split(jax.random.fold_in(key_list[6], part), 7)
    queries = draw_queries(jax.random.fold_in(jax.random.fold_in(key_list[6], part), 71), part)
    key_rows = draw_key_rows(jax.random.fold_in(jax.random.fold_in(key_list[6], part), 71), part)
    values = normal_values(own_keys[2], (RELAY_SECTIONS, SECTION_TOKENS, LOCAL_KV_HEADS * HEAD_SIZE), 1.0, 6.0, ((0, 2), (1, 4), (2, 2)))
    lengths = jax.vmap(lambda own: ragged_sizes(own, REQS, PAGES, MOST_PAGES, 2))(jax.random.split(own_keys[3], RELAY_SECTIONS)).reshape((RELAY_SECTIONS, REQS)).astype(jnp.int32)
    block_order = jax.vmap(lambda own: jax.random.permutation(own, N_SEQ))(jax.random.split(own_keys[4], RELAY_SECTIONS)).reshape((RELAY_SECTIONS, N_SEQ)).astype(jnp.int32)
    page_owner_keys = jax.random.split(jax.random.fold_in(own_keys[5], 1), RELAY_SECTIONS * PAGES // DEVICE_PAGES)
    page_owner_turns = jax.random.permutation(jax.random.fold_in(own_keys[5], 3), RELAY_SECTIONS * PAGES // DEVICE_PAGES)
    page_owner = jax.vmap(lambda own, number: shared_out(jax.random.fold_in(own_keys[5], 2), own, number, DEVICE_PAGES, N_SEQ, 1, SOURCE_SLOTS, 2))(page_owner_keys, page_owner_turns).reshape((RELAY_SECTIONS, PAGES, 1))
    return dict(queries=queries, key_rows=key_rows, values=values, lengths=lengths, block_order=block_order, page_owner=page_owner)


def reference(queries, key_rows, values, lengths, block_order, page_owner):
    query_group_width = QUERY_HEADS // LOCAL_KV_HEADS
    query_tile_rows = math.gcd(SECTION_TOKENS, 512)
    block_count = SECTION_TOKENS // query_tile_rows
    inv_root = 1.0 / math.sqrt(HEAD_SIZE)
    row_index = jnp.arange(SECTION_TOKENS, dtype=jnp.int32)

    def attention_section(inputs):
        section_queries, relay_key_rows, relay_value_rows, section_lengths, section_blocks = inputs
        starts = jnp.cumsum(section_lengths) - section_lengths
        position = (section_blocks[row_index // TOK_DEV] * TOK_DEV + row_index % TOK_DEV).astype(jnp.int32)
        request = lax.optimization_barrier(jnp.sum((position[:, None] // PAGE_TOKENS >= starts[None, :]).astype(jnp.int32), axis=1)) - 1
        per_head_keys = relay_key_rows.astype(jnp.float32).reshape(SECTION_TOKENS, LOCAL_KV_HEADS, HEAD_SIZE)
        per_head_values = relay_value_rows.astype(jnp.float32).reshape(SECTION_TOKENS, LOCAL_KV_HEADS, HEAD_SIZE)

        def query_part(items):
            slice_query_rows, part_pos, part_req = items
            head_split = slice_query_rows.astype(jnp.float32).reshape(query_tile_rows, LOCAL_KV_HEADS, query_group_width, HEAD_SIZE)
            scores = jnp.einsum('qgjd,kgd->qgjk', head_split, per_head_keys, precision=lax.Precision.HIGHEST) * inv_root
            allowed = ((request[None, :] == part_req[:, None]) & (position[None, :] <= part_pos[:, None]))[:, None, None, :]
            scores = jnp.where(allowed, scores, -1e+30)
            highest = lax.optimization_barrier(jnp.max(scores, axis=-1, keepdims=True))
            weights = jnp.where(allowed, jnp.exp(scores - highest), 0.0)
            total = lax.optimization_barrier(jnp.sum(weights, axis=-1))
            rounded = lax.optimization_barrier(weights.astype(jnp.bfloat16)).astype(jnp.float32)
            mixed = jnp.einsum('qgjk,kgd->qgjd', rounded, per_head_values, precision=lax.Precision.HIGHEST) / total[..., None]
            return mixed.reshape(query_tile_rows, QUERY_HEADS * HEAD_SIZE).astype(jnp.bfloat16)
        pieces = lax.map(query_part, (section_queries.reshape(block_count, query_tile_rows, QUERY_HEADS * HEAD_SIZE), position.reshape(block_count, query_tile_rows), request.reshape(block_count, query_tile_rows)))
        return pieces.reshape(SECTION_TOKENS, QUERY_HEADS * HEAD_SIZE)
    context = lax.map(attention_section, (queries, key_rows, values, lengths, block_order))
    handed = jnp.roll(context, 1, axis=0)

    def cache_section(inputs):
        relay_key_rows, relay_value_rows, section_blocks, section_owner = inputs
        owners = section_owner[:, 0].reshape(N_SEQ, DEVICE_PAGES)[section_blocks]
        page_index = jnp.arange(DEVICE_PAGES, dtype=jnp.int32)
        earlier = (owners[:, None, :] == owners[:, :, None]) & (page_index[None, :] < page_index[:, None])[None]
        slot_rank = lax.optimization_barrier(jnp.sum(earlier.astype(jnp.int32), axis=2))
        sources = jnp.arange(N_SEQ, dtype=jnp.int32)[:, None]
        destination_slot = (owners * (N_SEQ * SOURCE_SLOTS) + sources * SOURCE_SLOTS + slot_rank).reshape(-1).astype(jnp.int32)
        paged_key_cache = relay_key_rows.reshape(N_SEQ * DEVICE_PAGES, PAGE_TOKENS * LOCAL_KV_HEADS * HEAD_SIZE)
        paged_value_cache = relay_value_rows.reshape(N_SEQ * DEVICE_PAGES, PAGE_TOKENS * LOCAL_KV_HEADS * HEAD_SIZE)
        blank_pages = jnp.zeros((N_SEQ * N_SEQ * SOURCE_SLOTS, PAGE_TOKENS * LOCAL_KV_HEADS * HEAD_SIZE), jnp.bfloat16)
        cache_key_rows = blank_pages.at[destination_slot].set(paged_key_cache).reshape(N_SEQ, OWNER_CACHE_ROWS, LOCAL_KV_HEADS * HEAD_SIZE)
        cache_value_rows = blank_pages.at[destination_slot].set(paged_value_cache).reshape(N_SEQ, OWNER_CACHE_ROWS, LOCAL_KV_HEADS * HEAD_SIZE)
        return (cache_key_rows, cache_value_rows)
    cache_keys, cache_values = lax.map(cache_section, (key_rows, values, block_order, page_owner))
    return (handed, cache_keys, cache_values)
```

```python
import functools
import math

import jax
import jax.numpy as jnp
from jax import lax
from jax.experimental import pallas as pl
from jax.experimental.pallas import tpu as pltpu
from jax.sharding import PartitionSpec as P

HEAD = 128
PAGE = 16
NEG = -1e30
MESH = pl.DeviceIdType.MESH


def greet(barrier, peer):
    pl.semaphore_signal(barrier, inc=1, device_id=peer, device_id_type=MESH)


def kernel(
    dims,
    lengths_hbm,
    order_hbm,
    owner_hbm,
    q_hbm,
    k_hbm,
    v_hbm,
    handed,
    ck,
    cv,
    q,
    kall,
    vall,
    bias,
    ctx,
    lengths,
    order,
    owner,
    meta_sem,
    in_sem,
    send_sem,
    recv_sem,
    hand_send,
    hand_recv,
):
    n, sections, tok, kv_heads, width, slots = dims
    pages = tok // PAGE
    me = lax.axis_index("seq")
    sec = lax.axis_index("section")
    right, left = me + 1, me - 1
    onward, before = lax.rem(sec + 1, sections), lax.rem(sec + sections - 1, sections)
    half = tok // 2

    def block(ref, g, index):
        rows = pl.ds(pl.multiple_of(index * tok, tok), tok)
        return ref.at[g, rows, pl.ds(0, HEAD)]

    loads = []
    for g in range(kv_heads):
        for t, (src, dst) in enumerate(((k_hbm, kall), (v_hbm, vall))):
            load = pltpu.make_async_copy(
                src.at[0, :, pl.ds(g * HEAD, HEAD)], block(dst, g, me), in_sem.at[2 * g + t]
            )
            load.start()
            loads.append(load)
    metas = []
    for src, dst in ((lengths_hbm, lengths), (order_hbm, order), (owner_hbm, owner)):
        metas.append(pltpu.make_async_copy(src, dst, meta_sem.at[len(metas)]))
        metas[-1].start()
    q_load = pltpu.make_async_copy(q_hbm.at[0], q, in_sem.at[2 * kv_heads])
    q_load.start()

    barrier = pltpu.get_barrier_semaphore()
    others = []
    if sections > 1:
        others.append({"section": onward})
    if sections > 2:
        others.append({"section": before})
    pl.when(me < n - 1)(lambda: greet(barrier, {"seq": right}))
    pl.when(me > 0)(lambda: greet(barrier, {"seq": left}))
    for peer in others:
        greet(barrier, peer)
    beside = jnp.where(me < n - 1, 1, 0) + jnp.where(me > 0, 1, 0)
    pl.semaphore_wait(barrier, beside + len(others))

    def sends(way, d):
        return (me < n - 1) & (me >= d - 1) if way == 0 else (me > 0) & (me <= n - d)

    def takes(way, d):
        return me >= d if way == 0 else me + d <= n - 1

    def line(way, g, d, t, arriving):
        shift = d if arriving else d - 1
        ref = block((kall, vall)[t], g, me - shift if way == 0 else me + shift)
        return pltpu.make_async_remote_copy(
            src_ref=ref,
            dst_ref=ref,
            send_sem=send_sem.at[way, g, d - 1, t],
            recv_sem=recv_sem.at[way, g, d - 1, t],
            device_id={"seq": right if way == 0 else left},
            device_id_type=MESH,
        )

    def start(g, ts=(0, 1)):
        for t in ts:
            for way in range(2):
                pl.when(sends(way, 1))(lambda: line(way, g, 1, t, False).start())

    def pass_on(g, d):
        for t in range(2):
            for way in range(2):

                @pl.when(sends(way, d + 1))
                def _():
                    line(way, g, d, t, True).wait_recv()
                    line(way, g, d + 1, t, False).start()

    def settle(g):
        for d in range(1, n):
            for t in range(2):
                for way in range(2):
                    ends = takes(way, d) & jnp.logical_not(sends(way, d + 1))
                    pl.when(ends)(lambda: line(way, g, d, t, True).wait_recv())

    loads[0].wait()
    loads[1].wait()
    start(0)
    for load in loads[2:]:
        load.wait()
    for g in range(1, kv_heads):
        start(g, (0,))

    vall[:, :, HEAD:] = jnp.ones((kv_heads, n * tok, HEAD), vall.dtype)
    for meta in metas:
        meta.wait()
    begins = [0]
    for r in range(lengths.shape[1] - 1):
        begins.append(begins[-1] + lengths[0, r])

    def request(position):
        page = position // PAGE
        total = jnp.zeros_like(position)
        for begin in begins[1:]:
            total = total + (page >= begin).astype(jnp.int32)
        return total

    q_pos = order[0, me] * tok + lax.broadcasted_iota(jnp.int32, (tok, 1), 0)
    q_req = request(q_pos)

    def mask(i, _):
        k_pos = order[0, i] * tok + lax.broadcasted_iota(jnp.int32, (1, tok), 1)
        allowed = (request(k_pos) == q_req) & (k_pos <= q_pos)
        bias[:, pl.ds(pl.multiple_of(i * tok, tok), tok)] = jnp.where(allowed, 0.0, NEG)
        return 0

    lax.fori_loop(0, n, mask, 0)
    q_load.wait()

    for d in range(1, n - 1):
        pass_on(0, d)
    for g in range(1, kv_heads):
        start(g, (1,))
    settle(0)

    factor = math.log2(math.e) / math.sqrt(HEAD)

    def hand(h):
        cols = pl.ds(pl.multiple_of(h * HEAD, HEAD), HEAD)
        return pltpu.make_async_remote_copy(
            src_ref=ctx.at[:, cols],
            dst_ref=handed.at[:, cols],
            send_sem=hand_send.at[h],
            recv_sem=hand_recv.at[h],
            device_id={"section": onward},
            device_id_type=MESH,
        )

    def heads(g, low, high):
        def one(j, _):
            h = g * width + j
            cols = pl.ds(pl.multiple_of(h * HEAD, HEAD), HEAD)
            for part in range(2):
                rows = pl.ds(part * half, half)
                score = lax.dot_general(
                    q[rows, cols],
                    kall[g],
                    (((1,), (1,)), ((), ())),
                    preferred_element_type=jnp.float32,
                )
                score = score * factor + bias[rows, :]
                top = jnp.max(score, axis=1, keepdims=True)
                weight = jnp.exp2(score - top).astype(jnp.bfloat16)
                mixed = jnp.dot(weight, vall[g], preferred_element_type=jnp.float32)
                ctx[rows, cols] = (mixed[:, :HEAD] / mixed[:, HEAD:]).astype(ctx.dtype)
            hand(h).start()
            return 0

        lax.fori_loop(low, high, one, 0)

    for g in range(kv_heads):
        last = g + 1 == kv_heads
        for low in range(0, width, 2):
            heads(g, low, min(low + 2, width))
            d = low // 2 + 1
            if not last and d < n - 1 and low + 2 < width:
                pass_on(g + 1, d)
        if not last:
            for d in range((width - 1) // 2 + 1, n - 1):
                pass_on(g + 1, d)
            settle(g + 1)

    taken = slots * PAGE
    lane_page = lax.broadcasted_iota(jnp.int32, (1, tok), 1) // PAGE
    lane_token = lax.broadcasted_iota(jnp.int32, (1, tok), 1) % PAGE

    def pick(i, _):
        base = order[0, i] * pages
        target = jnp.full((1, tok), -1, jnp.int32)
        rank = jnp.int32(0)
        for p in range(pages):
            mine = owner[0, base + p] == me
            target = jnp.where(lane_page == p, jnp.where(mine, rank * PAGE, -taken), target)
            rank = rank + mine.astype(jnp.int32)
        target = target + lane_token
        select = (lax.broadcasted_iota(jnp.int32, (taken, tok), 0) == target).astype(jnp.bfloat16)
        rows = pl.ds(pl.multiple_of(i * tok, tok), tok)
        outs = pl.ds(pl.multiple_of(i * taken, taken), taken)
        for g in range(kv_heads):
            cols = pl.ds(g * HEAD, HEAD)
            for dst, src in ((ck, kall), (cv, vall)):
                dst[outs, cols] = jnp.dot(
                    select, src[g, rows, :HEAD], preferred_element_type=jnp.float32
                ).astype(dst.dtype)
        return 0

    lax.fori_loop(0, n, pick, 0)
    for g in range(kv_heads):
        for d in range(1, n):
            for t in range(2):
                for way in range(2):
                    pl.when(sends(way, d))(lambda: line(way, g, d, t, False).wait_send())

    def finish(h, _):
        copy = hand(h)
        copy.wait_send()
        copy.wait_recv()
        return 0

    lax.fori_loop(0, kv_heads * width, finish, 0)


def store(handed_v, ck_v, cv_v, handed, ck, cv, sem):
    copies = []
    for src, dst in ((handed_v, handed), (ck_v, ck), (cv_v, cv)):
        rows = src.shape[0] // 2
        view = dst.at[0] if dst.ndim == 3 else dst.at[0, 0]
        for part in range(2):
            piece = pl.ds(part * rows, rows)
            copies.append(
                pltpu.make_async_copy(src.at[piece], view.at[piece], sem.at[len(copies)])
            )
    for copy in copies:
        copy.start()
    for copy in copies:
        copy.wait()


def body(queries, key_rows, values, lengths, block_order, page_owner):
    n, sections = lax.axis_size("seq"), lax.axis_size("section")
    tok = key_rows.shape[1]
    kv_heads = key_rows.shape[2] // HEAD
    heads = queries.shape[2] // HEAD
    slots = max(2, 2 * (tok // PAGE) // n)
    dims = (n, sections, tok, kv_heads, heads // kv_heads, slots)
    steps = max(n - 1, 1)
    taken = n * slots * PAGE
    dtype = queries.dtype
    hbm = pl.BlockSpec(memory_space=pltpu.HBM)
    metas = lengths, block_order, page_owner.reshape(page_owner.shape[:2])
    vmem = pl.BlockSpec(memory_space=pltpu.VMEM)
    width = key_rows.shape[2]
    held = pl.pallas_call(
        functools.partial(kernel, dims),
        out_shape=(
            pltpu.VMEM(queries.shape[1:], dtype),
            pltpu.VMEM((taken, width), dtype),
            pltpu.VMEM((taken, width), dtype),
        ),
        in_specs=[hbm] * 6,
        out_specs=(vmem, vmem, vmem),
        scratch_shapes=[
            pltpu.VMEM((tok, heads * HEAD), dtype),
            pltpu.VMEM((kv_heads, n * tok, HEAD), dtype),
            pltpu.VMEM((kv_heads, n * tok, 2 * HEAD), dtype),
            pltpu.VMEM((tok, n * tok), jnp.float32),
            pltpu.VMEM((tok, heads * HEAD), dtype),
            *(pltpu.SMEM(x.shape, x.dtype) for x in metas),
            pltpu.SemaphoreType.DMA((3,)),
            pltpu.SemaphoreType.DMA((2 * kv_heads + 1,)),
            pltpu.SemaphoreType.DMA((2, kv_heads, steps, 2)),
            pltpu.SemaphoreType.DMA((2, kv_heads, steps, 2)),
            pltpu.SemaphoreType.DMA((heads,)),
            pltpu.SemaphoreType.DMA((heads,)),
        ],
        compiler_params=pltpu.CompilerParams(
            collective_id=0, has_side_effects=True, vmem_limit_bytes=48 << 20
        ),
    )(
        *(
            pltpu.with_memory_space_constraint(x, pltpu.HBM)
            for x in (*metas, queries, key_rows, values)
        ),
    )
    return pl.pallas_call(
        store,
        out_shape=(
            jax.ShapeDtypeStruct(queries.shape, dtype),
            jax.ShapeDtypeStruct((1, 1, taken, width), dtype),
            jax.ShapeDtypeStruct((1, 1, taken, width), dtype),
        ),
        in_specs=[vmem, vmem, vmem],
        out_specs=(hbm, hbm, hbm),
        scratch_shapes=[pltpu.SemaphoreType.DMA((6,))],
        compiler_params=pltpu.CompilerParams(vmem_limit_bytes=8 << 20),
    )(*(pltpu.with_memory_space_constraint(x, pltpu.VMEM) for x in held))


def solution(mesh):
    in_specs = (
        P(("groups", "section"), "seq", "kv"),
        P(("groups", "section"), "seq", "kv"),
        P(("groups", "section"), "seq", "kv"),
        P(("groups", "section"), None),
        P(("groups", "section"), None),
        P(("groups", "section"), None, None),
    )
    out_specs = (
        P(("groups", "section"), "seq", "kv"),
        P(("groups", "section"), "seq", None, "kv"),
        P(("groups", "section"), "seq", None, "kv"),
    )
    return jax.shard_map(body, mesh=mesh, in_specs=in_specs, out_specs=out_specs, check_vma=False)
```

```python
import functools
import math

import jax
import jax.numpy as jnp
from jax import lax
from jax.experimental import pallas as pl
from jax.experimental.pallas import tpu as pltpu
from jax.sharding import PartitionSpec as P

HEAD = 128
PAGE = 16
NEG = -1e30
MESH = pl.DeviceIdType.MESH


def kernel(
    dims,
    lengths_hbm,
    order_hbm,
    owner_hbm,
    q_hbm,
    k_hbm,
    v_hbm,
    handed,
    ck,
    cv,
    q,
    kall,
    vall,
    mates,
    bias,
    ctx,
    lengths,
    order,
    owner,
    meta_sem,
    in_sem,
    upper_sem,
    next_sem,
    push_send,
    push_recv,
    own_send,
    relay_send,
    recv_sem,
    hand_send,
    hand_recv,
):
    n, sections, cores, tok, kv_heads, width, slots = dims
    pages = tok // PAGE
    me = lax.axis_index("seq")
    sec = lax.axis_index("section")
    core = lax.axis_index("kv")
    onward = lax.rem(sec + 1, sections)
    half = tok // 2
    last = n - 1
    first_core = core == 0

    def head_cols(g):
        return pl.ds(g * HEAD, HEAD)

    def block(t, g, index):
        rows = pl.ds(pl.multiple_of(index * tok, tok), tok)
        return (kall, vall)[t].at[g, rows, pl.ds(0, HEAD)]

    loads = []
    for g in range(kv_heads):
        for t, src in enumerate((k_hbm, v_hbm)):
            load = pltpu.make_async_copy(
                src.at[0, :, head_cols(g)], block(t, g, me), in_sem.at[2 * g + t]
            )
            load.start()
            loads.append(load)
    metas = []
    for src, dst in ((lengths_hbm, lengths), (order_hbm, order), (owner_hbm, owner)):
        metas.append(pltpu.make_async_copy(src, dst, meta_sem.at[len(metas)]))
        metas[-1].start()
    q_load = pltpu.make_async_copy(q_hbm.at[0], q, in_sem.at[2 * kv_heads])
    q_load.start()

    barrier = pltpu.get_barrier_semaphore()
    for c in range(cores):

        @pl.when(core != c)
        def _():
            pl.semaphore_signal(barrier, inc=1, device_id={"kv": c}, device_id_type=MESH)

    below = jnp.where(me > 0, 1, 0) + jnp.where(sec > 0, 1, 0)
    pl.semaphore_wait(barrier, below + (cores - 1))

    @pl.when(me < last)
    def _():
        pl.semaphore_signal(barrier, inc=1, device_id={"seq": me + 1}, device_id_type=MESH)

    @pl.when(sec < sections - 1)
    def _():
        pl.semaphore_signal(barrier, inc=1, device_id={"section": sec + 1}, device_id_type=MESH)

    for j in range(last):

        @pl.when(j < me)
        def _():
            pl.semaphore_signal(
                upper_sem.at[me], inc=1, device_id={"seq": j}, device_id_type=MESH
            )

    @pl.when(sec > 0)
    def _():
        pl.semaphore_signal(next_sem, inc=1, device_id={"section": sec - 1}, device_id_type=MESH)

    units = [(c, g) for g in range(kv_heads) for c in range(cores)]
    inner = (me > 0) & (me < last)

    def gate(j):
        return 1 if j == 0 else n - 2

    def goes(u, j):
        if 0 < j < last:
            return me != j
        straight = me == gate(j)
        if u == 0 and j == 0 and gate(0) != last:
            straight = straight | (me == last)
        return straight

    def relays(g, b):
        found = []
        for j in (0, last):
            if b in (j, gate(j)):
                continue
            cond = me == gate(j)
            if g == 0 and j == 0 and b == last:
                cond = cond & jnp.logical_not(first_core)
            found.append((j, cond))
        return found

    def push(c, g, t):
        return pltpu.make_async_remote_copy(
            src_ref=(k_hbm, v_hbm)[t].at[0, :, head_cols(g)],
            dst_ref=mates.at[c - 1, g, t],
            send_sem=push_send.at[g, t],
            recv_sem=push_recv.at[c - 1, g, t],
            device_id={"kv": 0},
            device_id_type=MESH,
        )

    def own(u, j, t):
        c, g = units[u]
        src = mates.at[c - 1, g, t] if c else (k_hbm, v_hbm)[t].at[0, :, head_cols(g)]
        return pltpu.make_async_remote_copy(
            src_ref=src,
            dst_ref=block(t, g, me),
            send_sem=own_send.at[u, j, t],
            recv_sem=recv_sem.at[g, me, t],
            device_id={"seq": j, "kv": c},
            device_id_type=MESH,
        )

    def relay(g, b, j, t):
        ref = block(t, g, b)
        return pltpu.make_async_remote_copy(
            src_ref=ref,
            dst_ref=ref,
            send_sem=relay_send.at[g, b, t],
            recv_sem=recv_sem.at[g, b, t],
            device_id={"seq": j},
            device_id_type=MESH,
        )

    def send_own(u, j, cond):
        @pl.when(cond & goes(u, j))
        def _():
            for t in range(2):
                own(u, j, t).start()

    downward = sorted(
        ((u, j) for u in range(len(units)) for j in range(last)),
        key=lambda x: (x[0] + max(x[1] - 1, 0), x[1]),
    )
    upward = sorted(
        ((u, j) for u in range(len(units)) for j in range(1, n)),
        key=lambda x: (x[0], -x[1] if x[0] else x[1]),
    )

    @pl.when(jnp.logical_not(first_core))
    def _():
        for c in range(1, cores):

            @pl.when(core == c)
            def _():
                for g in range(kv_heads):
                    for t in range(2):
                        push(c, g, t).start()

    @pl.when(first_core)
    def _():
        here = set()
        for u, j in downward:
            c, g = units[u]
            if c and u not in here:
                here.add(u)
                for t in range(2):
                    push(c, g, t).wait_recv()
            early = (j < me) if u < cores else (j < me) & jnp.logical_not(inner)
            send_own(u, j, early)
        known = set()
        for u, j in upward:
            if j not in known:
                known.add(j)

                @pl.when((j > me) & goes(1, j))
                def _():
                    pl.semaphore_wait(upper_sem.at[j], 1)

            early = (j > me) if u < cores else (j > me) & jnp.logical_not(inner)
            send_own(u, j, early)

    for j in range(1, n):
        unknown = j > me
        unknown = unknown & (jnp.logical_not(first_core) | jnp.logical_not(goes(1, j)))

        @pl.when(unknown)
        def _():
            pl.semaphore_wait(upper_sem.at[j], 1)

    vall[:, :, HEAD:] = jnp.ones((kv_heads, n * tok, HEAD), vall.dtype)
    for meta in metas:
        meta.wait()
    begins = [0]
    for r in range(lengths.shape[1] - 1):
        begins.append(begins[-1] + lengths[0, r])

    def request(position):
        page = position // PAGE
        total = jnp.zeros_like(position)
        for begin in begins[1:]:
            total = total + (page >= begin).astype(jnp.int32)
        return total

    q_pos = order[0, me] * tok + lax.broadcasted_iota(jnp.int32, (tok, 1), 0)
    q_req = request(q_pos)

    def mask(i, _):
        k_pos = order[0, i] * tok + lax.broadcasted_iota(jnp.int32, (1, tok), 1)
        allowed = (request(k_pos) == q_req) & (k_pos <= q_pos)
        bias[:, pl.ds(pl.multiple_of(i * tok, tok), tok)] = jnp.where(allowed, 0.0, NEG)
        return 0

    lax.fori_loop(0, n, mask, 0)
    for load in loads:
        load.wait()
    q_load.wait()

    def pass_on(g, b):
        for j, cond in relays(g, b):

            @pl.when(cond)
            def _():
                for t in range(2):
                    relay(g, b, j, t).wait_recv()
                    relay(g, b, j, t).start()

    hops = {}
    for b in range(n):
        hops.setdefault(min(abs(b - gate(0)), abs(b - gate(last))), []).append(b)
    hops = [hops[d] for d in sorted(hops)]

    def settle(g):
        for b in range(n):
            arrives = me != b
            for _, cond in relays(g, b):
                arrives = arrives & jnp.logical_not(cond)

            @pl.when(arrives)
            def _():
                for t in range(2):
                    relay(g, b, 0, t).wait_recv()

    for blocks in hops:
        for b in blocks:
            pass_on(0, b)

    @pl.when(first_core & inner)
    def _():
        for u, j in downward:
            if u >= cores:
                send_own(u, j, j < me)
        for u, j in upward:
            if u >= cores:
                send_own(u, j, j > me)

    settle(0)

    @pl.when(sec < sections - 1)
    def _():
        pl.semaphore_wait(next_sem, 1)

    factor = math.log2(math.e) / math.sqrt(HEAD)

    def hand(h, part):
        rows = pl.ds(part * half, half)
        cols = pl.ds(pl.multiple_of(h * HEAD, HEAD), HEAD)
        return pltpu.make_async_remote_copy(
            src_ref=ctx.at[rows, cols],
            dst_ref=handed.at[rows, cols],
            send_sem=hand_send.at[h, part],
            recv_sem=hand_recv.at[h, part],
            device_id={"section": onward},
            device_id_type=MESH,
        )

    def heads(g, low, high):
        def one(j, _):
            h = g * width + j
            cols = pl.ds(pl.multiple_of(h * HEAD, HEAD), HEAD)
            for part in range(2):
                rows = pl.ds(part * half, half)
                score = lax.dot_general(
                    q[rows, cols],
                    kall[g],
                    (((1,), (1,)), ((), ())),
                    preferred_element_type=jnp.float32,
                )
                score = score * factor + bias[rows, :]
                top = jnp.max(score, axis=1, keepdims=True)
                weight = jnp.exp2(score - top).astype(jnp.bfloat16)
                mixed = jnp.dot(weight, vall[g], preferred_element_type=jnp.float32)
                ctx[rows, cols] = (mixed[:, :HEAD] / mixed[:, HEAD:]).astype(ctx.dtype)
                hand(h, part).start()
            return 0

        lax.fori_loop(low, high, one, 0)

    taken = slots * PAGE
    lane_page = lax.broadcasted_iota(jnp.int32, (1, tok), 1) // PAGE
    lane_token = lax.broadcasted_iota(jnp.int32, (1, tok), 1) % PAGE

    def keep(g):
        cols = head_cols(g)

        def pick(i, _):
            base = order[0, i] * pages
            target = jnp.full((1, tok), -1, jnp.int32)
            rank = jnp.int32(0)
            for p in range(pages):
                mine = owner[0, base + p] == me
                target = jnp.where(lane_page == p, jnp.where(mine, rank * PAGE, -taken), target)
                rank = rank + mine.astype(jnp.int32)
            target = target + lane_token
            select = lax.broadcasted_iota(jnp.int32, (taken, tok), 0) == target
            select = select.astype(jnp.bfloat16)
            rows = pl.ds(pl.multiple_of(i * tok, tok), tok)
            outs = pl.ds(pl.multiple_of(i * taken, taken), taken)
            for dst, src in ((ck, kall), (cv, vall)):
                dst[outs, cols] = jnp.dot(
                    select, src[g, rows, :HEAD], preferred_element_type=jnp.float32
                ).astype(dst.dtype)
            return 0

        lax.fori_loop(0, n, pick, 0)

    for g in range(kv_heads):
        low = 0
        if g + 1 < kv_heads:
            for i, blocks in enumerate(hops[:-1]):
                cut = (width + 1) // 2 + i * (width // 2) // len(hops)
                heads(g, low, cut)
                low = cut
                for b in blocks:
                    pass_on(g + 1, b)
        heads(g, low, width)
        keep(g)
        if g + 1 < kv_heads:
            for b in hops[-1]:
                pass_on(g + 1, b)
            settle(g + 1)

    for g in range(kv_heads):
        for b in range(n):
            for j, cond in relays(g, b):

                @pl.when(cond)
                def _():
                    for t in range(2):
                        relay(g, b, j, t).wait_send()

    @pl.when(first_core)
    def _():
        for u, j in downward:

            @pl.when((j < me) & goes(u, j))
            def _():
                for t in range(2):
                    own(u, j, t).wait_send()

        for u, j in upward:

            @pl.when((j > me) & goes(u, j))
            def _():
                for t in range(2):
                    own(u, j, t).wait_send()

    for c in range(1, cores):

        @pl.when(core == c)
        def _():
            for g in range(kv_heads):
                for t in range(2):
                    push(c, g, t).wait_send()

    def finish(h, _):
        for part in range(2):
            copy = hand(h, part)
            copy.wait_send()
            copy.wait_recv()
        return 0

    lax.fori_loop(0, kv_heads * width, finish, 0)


def store(handed_v, ck_v, cv_v, handed, ck, cv, sem):
    copies = []
    for src, dst in ((handed_v, handed), (ck_v, ck), (cv_v, cv)):
        rows = src.shape[0] // 2
        view = dst.at[0] if dst.ndim == 3 else dst.at[0, 0]
        for part in range(2):
            piece = pl.ds(part * rows, rows)
            copies.append(
                pltpu.make_async_copy(src.at[piece], view.at[piece], sem.at[len(copies)])
            )
    for copy in copies:
        copy.start()
    for copy in copies:
        copy.wait()


def body(queries, key_rows, values, lengths, block_order, page_owner):
    n, sections = lax.axis_size("seq"), lax.axis_size("section")
    cores = lax.axis_size("kv")
    tok, width = key_rows.shape[1:]
    kv_heads = width // HEAD
    heads = queries.shape[2] // HEAD
    slots = max(2, 2 * (tok // PAGE) // n)
    dims = (n, sections, cores, tok, kv_heads, heads // kv_heads, slots)
    taken = n * slots * PAGE
    dtype = queries.dtype
    metas = lengths, block_order, page_owner.reshape(page_owner.shape[:2])
    vmem = pl.BlockSpec(memory_space=pltpu.VMEM)
    hbm = pl.BlockSpec(memory_space=pltpu.HBM)
    dma = pltpu.SemaphoreType.DMA
    held = pl.pallas_call(
        functools.partial(kernel, dims),
        out_shape=(
            pltpu.VMEM(queries.shape[1:], dtype),
            pltpu.VMEM((taken, width), dtype),
            pltpu.VMEM((taken, width), dtype),
        ),
        in_specs=[hbm] * 6,
        out_specs=(vmem, vmem, vmem),
        scratch_shapes=[
            pltpu.VMEM((tok, heads * HEAD), dtype),
            pltpu.VMEM((kv_heads, n * tok, HEAD), dtype),
            pltpu.VMEM((kv_heads, n * tok, 2 * HEAD), dtype),
            pltpu.VMEM((max(cores - 1, 1), kv_heads, 2, tok, HEAD), dtype),
            pltpu.VMEM((tok, n * tok), jnp.float32),
            pltpu.VMEM((tok, heads * HEAD), dtype),
            *(pltpu.SMEM(x.shape, x.dtype) for x in metas),
            dma((3,)),
            dma((2 * kv_heads + 1,)),
            pltpu.SemaphoreType.REGULAR((n,)),
            pltpu.SemaphoreType.REGULAR,
            dma((kv_heads, 2)),
            dma((max(cores - 1, 1), kv_heads, 2)),
            dma((cores * kv_heads, n, 2)),
            dma((kv_heads, n, 2)),
            dma((kv_heads, n, 2)),
            dma((heads, 2)),
            dma((heads, 2)),
        ],
        compiler_params=pltpu.CompilerParams(
            collective_id=0, has_side_effects=True, vmem_limit_bytes=48 << 20
        ),
    )(
        *(
            pltpu.with_memory_space_constraint(x, pltpu.HBM)
            for x in (*metas, queries, key_rows, values)
        ),
    )
    return pl.pallas_call(
        store,
        out_shape=(
            jax.ShapeDtypeStruct(queries.shape, dtype),
            jax.ShapeDtypeStruct((1, 1, taken, width), dtype),
            jax.ShapeDtypeStruct((1, 1, taken, width), dtype),
        ),
        in_specs=[vmem, vmem, vmem],
        out_specs=(hbm, hbm, hbm),
        scratch_shapes=[dma((6,))],
        compiler_params=pltpu.CompilerParams(vmem_limit_bytes=8 << 20),
    )(*(pltpu.with_memory_space_constraint(x, pltpu.VMEM) for x in held))


def solution(mesh):
    in_specs = (
        P(("groups", "section"), "seq", "kv"),
        P(("groups", "section"), "seq", "kv"),
        P(("groups", "section"), "seq", "kv"),
        P(("groups", "section"), None),
        P(("groups", "section"), None),
        P(("groups", "section"), None, None),
    )
    out_specs = (
        P(("groups", "section"), "seq", "kv"),
        P(("groups", "section"), "seq", None, "kv"),
        P(("groups", "section"), "seq", None, "kv"),
    )
    return jax.shard_map(body, mesh=mesh, in_specs=in_specs, out_specs=out_specs, check_vma=False)
```

```python
import functools
import math

import jax
import jax.numpy as jnp
from jax import lax
from jax.experimental import pallas as pl
from jax.experimental.pallas import tpu as pltpu
from jax.sharding import PartitionSpec as P

HEAD = 128
PAGE = 16
NEG = -1e30
MESH = pl.DeviceIdType.MESH


def greet(barrier, peer):
    pl.semaphore_signal(barrier, inc=1, device_id=peer, device_id_type=MESH)


def kernel(
    dims,
    lengths_hbm,
    order_hbm,
    owner_hbm,
    q_hbm,
    k_hbm,
    v_hbm,
    handed,
    ck,
    cv,
    q,
    kall,
    vall,
    bias,
    ctx,
    lengths,
    order,
    owner,
    meta_sem,
    in_sem,
    send_sem,
    recv_sem,
    far_send,
    upper_sem,
    next_sem,
    hand_send,
    hand_recv,
):
    n, sections, cores, tok, kv_heads, width, slots = dims
    pages = tok // PAGE
    me = lax.axis_index("seq")
    sec = lax.axis_index("section")
    core = lax.axis_index("kv")
    right, left = me + 1, me - 1
    onward = lax.rem(sec + 1, sections)
    straight = n > 2
    half = tok // 2

    def block(ref, g, index):
        rows = pl.ds(pl.multiple_of(index * tok, tok), tok)
        return ref.at[g, rows, pl.ds(0, HEAD)]

    loads = []
    for g in range(kv_heads):
        for t, (src, dst) in enumerate(((k_hbm, kall), (v_hbm, vall))):
            load = pltpu.make_async_copy(
                src.at[0, :, pl.ds(g * HEAD, HEAD)], block(dst, g, me), in_sem.at[2 * g + t]
            )
            load.start()
            loads.append(load)
    metas = []
    for src, dst in ((lengths_hbm, lengths), (order_hbm, order), (owner_hbm, owner)):
        metas.append(pltpu.make_async_copy(src, dst, meta_sem.at[len(metas)]))
        metas[-1].start()
    q_load = pltpu.make_async_copy(q_hbm.at[0], q, in_sem.at[2 * kv_heads])
    q_load.start()

    barrier = pltpu.get_barrier_semaphore()
    below = jnp.where(me > 0, 1, 0) + jnp.where(sec > 0, 1, 0)
    pl.when(below > 0)(lambda: pl.semaphore_wait(barrier, below))
    pl.when(me < n - 1)(lambda: greet(barrier, {"seq": right}))
    pl.when(sec < sections - 1)(lambda: greet(barrier, {"section": sec + 1}))
    pl.when(me > 0)(lambda: greet(upper_sem, {"seq": left}))
    pl.when(sec > 0)(lambda: greet(next_sem, {"section": sec - 1}))

    def sends(way, g, d):
        if way == 0:
            return (me < n - 1) & (me >= d - 1)
        if straight and g == 0 and d == n - 1:
            return me < 0
        return (me > 0) & (me <= n - d)

    def takes(way, d):
        return me >= d if way == 0 else me + d <= n - 1

    def line(way, g, d, t, arriving):
        shift = d if arriving else d - 1
        ref = block((kall, vall)[t], g, me - shift if way == 0 else me + shift)
        src = ref
        if d == 1 and not arriving:
            src = (k_hbm, v_hbm)[t].at[0, :, pl.ds(g * HEAD, HEAD)]
        return pltpu.make_async_remote_copy(
            src_ref=src,
            dst_ref=ref,
            send_sem=send_sem.at[way, g, d - 1, t],
            recv_sem=recv_sem.at[way, g, d - 1, t],
            device_id={"seq": right if way == 0 else left},
            device_id_type=MESH,
        )

    def far(t):
        return pltpu.make_async_remote_copy(
            src_ref=(k_hbm, v_hbm)[t].at[0, :, pl.ds(0, HEAD)],
            dst_ref=block((kall, vall)[t], 0, me),
            send_sem=far_send.at[t],
            recv_sem=recv_sem.at[1, 0, n - 2, t],
            device_id={"seq": 0},
            device_id_type=MESH,
        )

    def start(way, g, ts=(0, 1)):
        for t in ts:
            pl.when(sends(way, g, 1))(lambda: line(way, g, 1, t, False).start())

    def pass_on(g, d):
        for t in range(2):
            for way in range(2):

                @pl.when(sends(way, g, d + 1))
                def _():
                    line(way, g, d, t, True).wait_recv()
                    line(way, g, d + 1, t, False).start()

    def settle(g):
        for d in range(1, n):
            for t in range(2):
                for way in range(2):
                    ends = takes(way, d) & jnp.logical_not(sends(way, g, d + 1))
                    pl.when(ends)(lambda: line(way, g, d, t, True).wait_recv())

    if straight:
        for t in range(2):
            pl.when(me == n - 1)(lambda: far(t).start())
    start(1, 0)
    for g in range(1, kv_heads):
        start(1, g, (0,))
    pl.when(me < n - 1)(lambda: pl.semaphore_wait(upper_sem, 1))
    start(0, 0)
    for g in range(1, kv_heads):
        start(0, g, (0,))

    vall[:, :, HEAD:] = jnp.ones((kv_heads, n * tok, HEAD), vall.dtype)
    for meta in metas:
        meta.wait()
    begins = [0]
    for r in range(lengths.shape[1] - 1):
        begins.append(begins[-1] + lengths[0, r])

    def request(position):
        page = position // PAGE
        total = jnp.zeros_like(position)
        for begin in begins[1:]:
            total = total + (page >= begin).astype(jnp.int32)
        return total

    q_pos = order[0, me] * tok + lax.broadcasted_iota(jnp.int32, (tok, 1), 0)
    q_req = request(q_pos)

    def mask(i, _):
        k_pos = order[0, i] * tok + lax.broadcasted_iota(jnp.int32, (1, tok), 1)
        allowed = (request(k_pos) == q_req) & (k_pos <= q_pos)
        bias[:, pl.ds(pl.multiple_of(i * tok, tok), tok)] = jnp.where(allowed, 0.0, NEG)
        return 0

    lax.fori_loop(0, n, mask, 0)

    for d in range(1, n - 1):
        pass_on(0, d)
    for g in range(1, kv_heads):
        for way in range(2):
            start(way, g, (1,))
    for load in loads:
        load.wait()
    q_load.wait()
    pl.when(sec < sections - 1)(lambda: pl.semaphore_wait(next_sem, 1))
    settle(0)

    factor = math.log2(math.e) / math.sqrt(HEAD)

    def hand(h):
        cols = pl.ds(pl.multiple_of(h * HEAD, HEAD), HEAD)
        return pltpu.make_async_remote_copy(
            src_ref=ctx.at[:, cols],
            dst_ref=handed.at[:, cols],
            send_sem=hand_send.at[h],
            recv_sem=hand_recv.at[h],
            device_id={"section": onward},
            device_id_type=MESH,
        )

    def heads(g, low, high):
        for part in range(2):
            rows = pl.ds(part * half, half)
            for h in range(g * width + low, g * width + high):
                cols = pl.ds(h * HEAD, HEAD)
                score = lax.dot_general(
                    q[rows, cols],
                    kall[g],
                    (((1,), (1,)), ((), ())),
                    preferred_element_type=jnp.float32,
                )
                score = score * factor + bias[rows, :]
                top = jnp.max(score, axis=1, keepdims=True)
                weight = jnp.exp2(score - top).astype(jnp.bfloat16)
                mixed = jnp.dot(weight, vall[g], preferred_element_type=jnp.float32)
                ctx[rows, cols] = (mixed[:, :HEAD] / mixed[:, HEAD:]).astype(ctx.dtype)
        for h in range(g * width + low, g * width + high):
            hand(h).start()

    for g in range(kv_heads):
        last = g + 1 == kv_heads
        for low in range(0, width, 2):
            heads(g, low, min(low + 2, width))
            d = low // 2 + 1
            if not last and d < n - 1 and low + 2 < width:
                pass_on(g + 1, d)
        if not last:
            for d in range((width - 1) // 2 + 1, n - 1):
                pass_on(g + 1, d)
            settle(g + 1)

    taken = slots * PAGE
    lane_page = lax.broadcasted_iota(jnp.int32, (1, tok), 1) // PAGE
    lane_token = lax.broadcasted_iota(jnp.int32, (1, tok), 1) % PAGE

    def pick(i, _):
        base = order[0, i] * pages
        target = jnp.full((1, tok), -1, jnp.int32)
        rank = jnp.int32(0)
        for p in range(pages):
            mine = owner[0, base + p] == me
            target = jnp.where(lane_page == p, jnp.where(mine, rank * PAGE, -taken), target)
            rank = rank + mine.astype(jnp.int32)
        target = target + lane_token
        select = (lax.broadcasted_iota(jnp.int32, (taken, tok), 0) == target).astype(jnp.bfloat16)
        rows = pl.ds(pl.multiple_of(i * tok, tok), tok)
        outs = pl.ds(pl.multiple_of(i * taken, taken), taken)
        for g in range(kv_heads):
            cols = pl.ds(g * HEAD, HEAD)
            for dst, src in ((ck, kall), (cv, vall)):
                dst[outs, cols] = jnp.dot(
                    select, src[g, rows, :HEAD], preferred_element_type=jnp.float32
                ).astype(dst.dtype)
        return 0

    lax.fori_loop(0, n, pick, 0)
    for g in range(kv_heads):
        for d in range(1, n):
            for t in range(2):
                for way in range(2):
                    pl.when(sends(way, g, d))(lambda: line(way, g, d, t, False).wait_send())

    if straight:
        for t in range(2):
            pl.when(me == n - 1)(lambda: far(t).wait_send())

    def finish(h, _):
        copy = hand(h)
        copy.wait_send()
        copy.wait_recv()
        return 0

    lax.fori_loop(0, kv_heads * width, finish, 0)


def store(handed_v, ck_v, cv_v, handed, ck, cv, sem):
    copies = []
    for src, dst in ((handed_v, handed), (ck_v, ck), (cv_v, cv)):
        rows = src.shape[0] // 2
        view = dst.at[0] if dst.ndim == 3 else dst.at[0, 0]
        for part in range(2):
            piece = pl.ds(part * rows, rows)
            copies.append(
                pltpu.make_async_copy(src.at[piece], view.at[piece], sem.at[len(copies)])
            )
    for copy in copies:
        copy.start()
    for copy in copies:
        copy.wait()


def body(queries, key_rows, values, lengths, block_order, page_owner):
    n, sections = lax.axis_size("seq"), lax.axis_size("section")
    tok = key_rows.shape[1]
    kv_heads = key_rows.shape[2] // HEAD
    heads = queries.shape[2] // HEAD
    slots = max(2, 2 * (tok // PAGE) // n)
    cores = lax.axis_size("kv")
    dims = (n, sections, cores, tok, kv_heads, heads // kv_heads, slots)
    steps = max(n - 1, 1)
    taken = n * slots * PAGE
    dtype = queries.dtype
    hbm = pl.BlockSpec(memory_space=pltpu.HBM)
    metas = lengths, block_order, page_owner.reshape(page_owner.shape[:2])
    vmem = pl.BlockSpec(memory_space=pltpu.VMEM)
    width = key_rows.shape[2]
    held = pl.pallas_call(
        functools.partial(kernel, dims),
        out_shape=(
            pltpu.VMEM(queries.shape[1:], dtype),
            pltpu.VMEM((taken, width), dtype),
            pltpu.VMEM((taken, width), dtype),
        ),
        in_specs=[hbm] * 6,
        out_specs=(vmem, vmem, vmem),
        scratch_shapes=[
            pltpu.VMEM((tok, heads * HEAD), dtype),
            pltpu.VMEM((kv_heads, n * tok, HEAD), dtype),
            pltpu.VMEM((kv_heads, n * tok, 2 * HEAD), dtype),
            pltpu.VMEM((tok, n * tok), jnp.float32),
            pltpu.VMEM((tok, heads * HEAD), dtype),
            *(pltpu.SMEM(x.shape, x.dtype) for x in metas),
            pltpu.SemaphoreType.DMA((3,)),
            pltpu.SemaphoreType.DMA((2 * kv_heads + 1,)),
            pltpu.SemaphoreType.DMA((2, kv_heads, steps, 2)),
            pltpu.SemaphoreType.DMA((2, kv_heads, steps, 2)),
            pltpu.SemaphoreType.DMA((2,)),
            pltpu.SemaphoreType.REGULAR,
            pltpu.SemaphoreType.REGULAR,
            pltpu.SemaphoreType.DMA((heads,)),
            pltpu.SemaphoreType.DMA((heads,)),
        ],
        compiler_params=pltpu.CompilerParams(
            collective_id=0, has_side_effects=True, vmem_limit_bytes=48 << 20
        ),
    )(
        *(
            pltpu.with_memory_space_constraint(x, pltpu.HBM)
            for x in (*metas, queries, key_rows, values)
        ),
    )
    return pl.pallas_call(
        store,
        out_shape=(
            jax.ShapeDtypeStruct(queries.shape, dtype),
            jax.ShapeDtypeStruct((1, 1, taken, width), dtype),
            jax.ShapeDtypeStruct((1, 1, taken, width), dtype),
        ),
        in_specs=[vmem, vmem, vmem],
        out_specs=(hbm, hbm, hbm),
        scratch_shapes=[pltpu.SemaphoreType.DMA((6,))],
        compiler_params=pltpu.CompilerParams(vmem_limit_bytes=8 << 20),
    )(*(pltpu.with_memory_space_constraint(x, pltpu.VMEM) for x in held))


def solution(mesh):
    in_specs = (
        P(("groups", "section"), "seq", "kv"),
        P(("groups", "section"), "seq", "kv"),
        P(("groups", "section"), "seq", "kv"),
        P(("groups", "section"), None),
        P(("groups", "section"), None),
        P(("groups", "section"), None, None),
    )
    out_specs = (
        P(("groups", "section"), "seq", "kv"),
        P(("groups", "section"), "seq", None, "kv"),
        P(("groups", "section"), "seq", None, "kv"),
    )
    return jax.shard_map(body, mesh=mesh, in_specs=in_specs, out_specs=out_specs, check_vma=False)
```

```python
import functools
import math

import jax
import jax.numpy as jnp
from jax import lax
from jax.experimental import pallas as pl
from jax.experimental.pallas import tpu as pltpu
from jax.sharding import PartitionSpec as P

HEAD = 128
PAGE = 16
NEG = -1e30
MESH = pl.DeviceIdType.MESH


def greet(barrier, peer):
    pl.semaphore_signal(barrier, inc=1, device_id=peer, device_id_type=MESH)


def kernel(
    dims,
    lengths_hbm,
    order_hbm,
    owner_hbm,
    q_hbm,
    k_hbm,
    v_hbm,
    handed,
    ck,
    cv,
    q,
    kall,
    vall,
    bias,
    weights,
    ctx,
    lengths,
    order,
    owner,
    meta_sem,
    in_sem,
    send_sem,
    recv_sem,
    far_send,
    upper_sem,
    next_sem,
    hand_send,
    hand_recv,
):
    n, sections, cores, tok, kv_heads, width, slots = dims
    pages = tok // PAGE
    me = lax.axis_index("seq")
    sec = lax.axis_index("section")
    core = lax.axis_index("kv")
    right, left = me + 1, me - 1
    onward = lax.rem(sec + 1, sections)
    straight = n > 2
    half = tok // 2

    def block(ref, g, index):
        rows = pl.ds(pl.multiple_of(index * tok, tok), tok)
        return ref.at[g, rows, pl.ds(0, HEAD)]

    loads = []
    for g in range(kv_heads):
        for t, (src, dst) in enumerate(((k_hbm, kall), (v_hbm, vall))):
            load = pltpu.make_async_copy(
                src.at[0, :, pl.ds(g * HEAD, HEAD)], block(dst, g, me), in_sem.at[2 * g + t]
            )
            load.start()
            loads.append(load)
    metas = []
    for src, dst in ((lengths_hbm, lengths), (order_hbm, order), (owner_hbm, owner)):
        metas.append(pltpu.make_async_copy(src, dst, meta_sem.at[len(metas)]))
        metas[-1].start()
    q_load = pltpu.make_async_copy(q_hbm.at[0], q, in_sem.at[2 * kv_heads])
    q_load.start()

    barrier = pltpu.get_barrier_semaphore()
    below = jnp.where(me > 0, 1, 0) + jnp.where(sec > 0, 1, 0)
    pl.when(below > 0)(lambda: pl.semaphore_wait(barrier, below))
    pl.when(me < n - 1)(lambda: greet(barrier, {"seq": right}))
    pl.when(sec < sections - 1)(lambda: greet(barrier, {"section": sec + 1}))
    pl.when(me > 0)(lambda: greet(upper_sem, {"seq": left}))
    pl.when(sec > 0)(lambda: greet(next_sem, {"section": sec - 1}))

    def sends(way, g, d):
        if way == 0:
            return (me < n - 1) & (me >= d - 1)
        if straight and g == 0 and d == n - 1:
            return me < 0
        return (me > 0) & (me <= n - d)

    def takes(way, d):
        return me >= d if way == 0 else me + d <= n - 1

    def line(way, g, d, t, arriving):
        shift = d if arriving else d - 1
        ref = block((kall, vall)[t], g, me - shift if way == 0 else me + shift)
        src = ref
        if d == 1 and not arriving:
            src = (k_hbm, v_hbm)[t].at[0, :, pl.ds(g * HEAD, HEAD)]
        return pltpu.make_async_remote_copy(
            src_ref=src,
            dst_ref=ref,
            send_sem=send_sem.at[way, g, d - 1, t],
            recv_sem=recv_sem.at[way, g, d - 1, t],
            device_id={"seq": right if way == 0 else left},
            device_id_type=MESH,
        )

    def far(t):
        return pltpu.make_async_remote_copy(
            src_ref=(k_hbm, v_hbm)[t].at[0, :, pl.ds(0, HEAD)],
            dst_ref=block((kall, vall)[t], 0, me),
            send_sem=far_send.at[t],
            recv_sem=recv_sem.at[1, 0, n - 2, t],
            device_id={"seq": 0},
            device_id_type=MESH,
        )

    def start(way, g, ts=(0, 1)):
        for t in ts:
            pl.when(sends(way, g, 1))(lambda: line(way, g, 1, t, False).start())

    def pass_on(g, d):
        for t in range(2):
            for way in range(2):

                @pl.when(sends(way, g, d + 1))
                def _():
                    line(way, g, d, t, True).wait_recv()
                    line(way, g, d + 1, t, False).start()

    def settle(g, t):
        for d in range(1, n):
            for way in range(2):
                ends = takes(way, d) & jnp.logical_not(sends(way, g, d + 1))
                pl.when(ends)(lambda: line(way, g, d, t, True).wait_recv())

    if straight:
        for t in range(2):
            pl.when(me == n - 1)(lambda: far(t).start())
    start(1, 0)
    for g in range(1, kv_heads):
        start(1, g, (0,))
    pl.when(me < n - 1)(lambda: pl.semaphore_wait(upper_sem, 1))
    start(0, 0)
    for g in range(1, kv_heads):
        start(0, g, (0,))

    vall[:, :, HEAD:] = jnp.ones((kv_heads, n * tok, HEAD), vall.dtype)
    for meta in metas:
        meta.wait()
    begins = [0]
    for r in range(lengths.shape[1] - 1):
        begins.append(begins[-1] + lengths[0, r])

    def request(position):
        page = position // PAGE
        total = jnp.zeros_like(position)
        for begin in begins[1:]:
            total = total + (page >= begin).astype(jnp.int32)
        return total

    q_pos = order[0, me] * tok + lax.broadcasted_iota(jnp.int32, (tok, 1), 0)
    q_req = request(q_pos)

    def mask(i, _):
        k_pos = order[0, i] * tok + lax.broadcasted_iota(jnp.int32, (1, tok), 1)
        allowed = (request(k_pos) == q_req) & (k_pos <= q_pos)
        bias[:, pl.ds(pl.multiple_of(i * tok, tok), tok)] = jnp.where(allowed, 0.0, NEG)
        return 0

    lax.fori_loop(0, n, mask, 0)

    for d in range(1, n - 1):
        pass_on(0, d)
    for g in range(1, kv_heads):
        for way in range(2):
            start(way, g, (1,))
    for load in loads:
        load.wait()
    q_load.wait()
    pl.when(sec < sections - 1)(lambda: pl.semaphore_wait(next_sem, 1))

    factor = math.log2(math.e) / math.sqrt(HEAD)

    def hand(h):
        cols = pl.ds(pl.multiple_of(h * HEAD, HEAD), HEAD)
        return pltpu.make_async_remote_copy(
            src_ref=ctx.at[:, cols],
            dst_ref=handed.at[:, cols],
            send_sem=hand_send.at[h],
            recv_sem=hand_recv.at[h],
            device_id={"section": onward},
            device_id_type=MESH,
        )

    def weigh(g, h, rows):
        score = lax.dot_general(
            q[rows, pl.ds(h * HEAD, HEAD)],
            kall[g],
            (((1,), (1,)), ((), ())),
            preferred_element_type=jnp.float32,
        )
        score = score * factor + bias[rows, :]
        top = jnp.max(score, axis=1, keepdims=True)
        return jnp.exp2(score - top).astype(jnp.bfloat16)

    def mix(g, h, rows, weight):
        mixed = jnp.dot(weight, vall[g], preferred_element_type=jnp.float32)
        mixed = mixed[:, :HEAD] / mixed[:, HEAD:]
        ctx[rows, pl.ds(h * HEAD, HEAD)] = mixed.astype(ctx.dtype)

    def heads(g, low, high):
        several = range(g * width + low, g * width + high)
        halves = [pl.ds(part * half, half) for part in range(2)]
        if low == 0:
            settle(g, 0)
            for rows in halves:
                for i, h in enumerate(several):
                    weights[i, rows, :] = weigh(g, h, rows)
            settle(g, 1)
            for rows in halves:
                for i, h in enumerate(several):
                    mix(g, h, rows, weights[i, rows, :])
        else:
            for rows in halves:
                for h in several:
                    mix(g, h, rows, weigh(g, h, rows))
        for h in several:
            hand(h).start()

    for g in range(kv_heads):
        last = g + 1 == kv_heads
        for low in range(0, width, 2):
            heads(g, low, min(low + 2, width))
            d = low // 2 + 1
            if not last and d < n - 1 and low + 2 < width:
                pass_on(g + 1, d)
        if not last:
            for d in range((width - 1) // 2 + 1, n - 1):
                pass_on(g + 1, d)

    taken = slots * PAGE
    lane_page = lax.broadcasted_iota(jnp.int32, (1, tok), 1) // PAGE
    lane_token = lax.broadcasted_iota(jnp.int32, (1, tok), 1) % PAGE

    def pick(i, _):
        base = order[0, i] * pages
        target = jnp.full((1, tok), -1, jnp.int32)
        rank = jnp.int32(0)
        for p in range(pages):
            mine = owner[0, base + p] == me
            target = jnp.where(lane_page == p, jnp.where(mine, rank * PAGE, -taken), target)
            rank = rank + mine.astype(jnp.int32)
        target = target + lane_token
        select = (lax.broadcasted_iota(jnp.int32, (taken, tok), 0) == target).astype(jnp.bfloat16)
        rows = pl.ds(pl.multiple_of(i * tok, tok), tok)
        outs = pl.ds(pl.multiple_of(i * taken, taken), taken)
        for g in range(kv_heads):
            cols = pl.ds(g * HEAD, HEAD)
            for dst, src in ((ck, kall), (cv, vall)):
                dst[outs, cols] = jnp.dot(
                    select, src[g, rows, :HEAD], preferred_element_type=jnp.float32
                ).astype(dst.dtype)
        return 0

    lax.fori_loop(0, n, pick, 0)
    for g in range(kv_heads):
        for d in range(1, n):
            for t in range(2):
                for way in range(2):
                    pl.when(sends(way, g, d))(lambda: line(way, g, d, t, False).wait_send())

    if straight:
        for t in range(2):
            pl.when(me == n - 1)(lambda: far(t).wait_send())

    def finish(h, _):
        copy = hand(h)
        copy.wait_send()
        copy.wait_recv()
        return 0

    lax.fori_loop(0, kv_heads * width, finish, 0)


def store(handed_v, ck_v, cv_v, handed, ck, cv, sem):
    copies = []
    for src, dst in ((handed_v, handed), (ck_v, ck), (cv_v, cv)):
        rows = src.shape[0] // 4
        view = dst.at[0] if dst.ndim == 3 else dst.at[0, 0]
        for part in range(4):
            piece = pl.ds(part * rows, rows)
            copies.append(
                pltpu.make_async_copy(src.at[piece], view.at[piece], sem.at[len(copies)])
            )
    for copy in copies:
        copy.start()
    for copy in copies:
        copy.wait()


def body(queries, key_rows, values, lengths, block_order, page_owner):
    n, sections = lax.axis_size("seq"), lax.axis_size("section")
    tok = key_rows.shape[1]
    kv_heads = key_rows.shape[2] // HEAD
    heads = queries.shape[2] // HEAD
    slots = max(2, 2 * (tok // PAGE) // n)
    cores = lax.axis_size("kv")
    dims = (n, sections, cores, tok, kv_heads, heads // kv_heads, slots)
    steps = max(n - 1, 1)
    taken = n * slots * PAGE
    dtype = queries.dtype
    hbm = pl.BlockSpec(memory_space=pltpu.HBM)
    metas = lengths, block_order, page_owner.reshape(page_owner.shape[:2])
    vmem = pl.BlockSpec(memory_space=pltpu.VMEM)
    width = key_rows.shape[2]
    held = pl.pallas_call(
        functools.partial(kernel, dims),
        out_shape=(
            pltpu.VMEM(queries.shape[1:], dtype),
            pltpu.VMEM((taken, width), dtype),
            pltpu.VMEM((taken, width), dtype),
        ),
        in_specs=[hbm] * 6,
        out_specs=(vmem, vmem, vmem),
        scratch_shapes=[
            pltpu.VMEM((tok, heads * HEAD), dtype),
            pltpu.VMEM((kv_heads, n * tok, HEAD), dtype),
            pltpu.VMEM((kv_heads, n * tok, 2 * HEAD), dtype),
            pltpu.VMEM((tok, n * tok), jnp.float32),
            pltpu.VMEM((2, tok, n * tok), dtype),
            pltpu.VMEM((tok, heads * HEAD), dtype),
            *(pltpu.SMEM(x.shape, x.dtype) for x in metas),
            pltpu.SemaphoreType.DMA((3,)),
            pltpu.SemaphoreType.DMA((2 * kv_heads + 1,)),
            pltpu.SemaphoreType.DMA((2, kv_heads, steps, 2)),
            pltpu.SemaphoreType.DMA((2, kv_heads, steps, 2)),
            pltpu.SemaphoreType.DMA((2,)),
            pltpu.SemaphoreType.REGULAR,
            pltpu.SemaphoreType.REGULAR,
            pltpu.SemaphoreType.DMA((heads,)),
            pltpu.SemaphoreType.DMA((heads,)),
        ],
        compiler_params=pltpu.CompilerParams(
            collective_id=0, has_side_effects=True, vmem_limit_bytes=48 << 20
        ),
    )(
        *(
            pltpu.with_memory_space_constraint(x, pltpu.HBM)
            for x in (*metas, queries, key_rows, values)
        ),
    )
    return pl.pallas_call(
        store,
        out_shape=(
            jax.ShapeDtypeStruct(queries.shape, dtype),
            jax.ShapeDtypeStruct((1, 1, taken, width), dtype),
            jax.ShapeDtypeStruct((1, 1, taken, width), dtype),
        ),
        in_specs=[vmem, vmem, vmem],
        out_specs=(hbm, hbm, hbm),
        scratch_shapes=[pltpu.SemaphoreType.DMA((12,))],
        compiler_params=pltpu.CompilerParams(vmem_limit_bytes=8 << 20),
    )(*(pltpu.with_memory_space_constraint(x, pltpu.VMEM) for x in held))


def solution(mesh):
    in_specs = (
        P(("groups", "section"), "seq", "kv"),
        P(("groups", "section"), "seq", "kv"),
        P(("groups", "section"), "seq", "kv"),
        P(("groups", "section"), None),
        P(("groups", "section"), None),
        P(("groups", "section"), None, None),
    )
    out_specs = (
        P(("groups", "section"), "seq", "kv"),
        P(("groups", "section"), "seq", None, "kv"),
        P(("groups", "section"), "seq", None, "kv"),
    )
    return jax.shard_map(body, mesh=mesh, in_specs=in_specs, out_specs=out_specs, check_vma=False)
```

```python
import functools
import math

import jax
import jax.numpy as jnp
from jax import lax
from jax.experimental import pallas as pl
from jax.experimental.pallas import tpu as pltpu
from jax.sharding import PartitionSpec as P

HEAD = 128
PAGE = 16
NEG = -1e30
MESH = pl.DeviceIdType.MESH


def greet(barrier, peer):
    pl.semaphore_signal(barrier, inc=1, device_id=peer, device_id_type=MESH)


def kernel(
    dims,
    lengths_hbm,
    order_hbm,
    owner_hbm,
    q_hbm,
    k_hbm,
    v_hbm,
    handed,
    ck,
    cv,
    q,
    kall,
    vall,
    bias,
    weights,
    ctx,
    lengths,
    order,
    owner,
    meta_sem,
    in_sem,
    send_sem,
    recv_sem,
    far_send,
    upper_sem,
    next_sem,
    hand_send,
    hand_recv,
):
    n, sections, cores, tok, kv_heads, width, slots = dims
    pages = tok // PAGE
    me = lax.axis_index("seq")
    sec = lax.axis_index("section")
    core = lax.axis_index("kv")
    right, left = me + 1, me - 1
    onward = lax.rem(sec + 1, sections)
    straight = n > 2
    half = tok // 2

    def block(ref, g, index):
        rows = pl.ds(pl.multiple_of(index * tok, tok), tok)
        return ref.at[g, rows, pl.ds(0, HEAD)]

    barrier = pltpu.get_barrier_semaphore()
    below = jnp.where(me > 0, 1, 0) + jnp.where(sec > 0, 1, 0)
    pl.when(below > 0)(lambda: pl.semaphore_wait(barrier, below))
    pl.when(me < n - 1)(lambda: greet(barrier, {"seq": right}))
    pl.when(sec < sections - 1)(lambda: greet(barrier, {"section": sec + 1}))
    pl.when(me > 0)(lambda: greet(upper_sem, {"seq": left}))
    pl.when(sec > 0)(lambda: greet(next_sem, {"section": sec - 1}))

    def sends(way, g, d):
        if way == 0:
            return (me < n - 1) & (me >= d - 1)
        if straight and g == 0 and d == n - 1:
            return me < 0
        return (me > 0) & (me <= n - d)

    def takes(way, d):
        return me >= d if way == 0 else me + d <= n - 1

    def line(way, g, d, t, arriving):
        shift = d if arriving else d - 1
        ref = block((kall, vall)[t], g, me - shift if way == 0 else me + shift)
        src = ref
        if d == 1 and not arriving:
            src = (k_hbm, v_hbm)[t].at[0, :, pl.ds(g * HEAD, HEAD)]
        return pltpu.make_async_remote_copy(
            src_ref=src,
            dst_ref=ref,
            send_sem=send_sem.at[way, g, d - 1, t],
            recv_sem=recv_sem.at[way, g, d - 1, t],
            device_id={"seq": right if way == 0 else left},
            device_id_type=MESH,
        )

    def far(t):
        return pltpu.make_async_remote_copy(
            src_ref=(k_hbm, v_hbm)[t].at[0, :, pl.ds(0, HEAD)],
            dst_ref=block((kall, vall)[t], 0, me),
            send_sem=far_send.at[t],
            recv_sem=recv_sem.at[1, 0, n - 2, t],
            device_id={"seq": 0},
            device_id_type=MESH,
        )

    def start(way, g, ts=(0, 1)):
        for t in ts:
            pl.when(sends(way, g, 1))(lambda: line(way, g, 1, t, False).start())

    def pass_on(g, d):
        for t in range(2):
            for way in range(2):

                @pl.when(sends(way, g, d + 1))
                def _():
                    line(way, g, d, t, True).wait_recv()
                    line(way, g, d + 1, t, False).start()

    def settle(g, t):
        for d in range(1, n):
            for way in range(2):
                ends = takes(way, d) & jnp.logical_not(sends(way, g, d + 1))
                pl.when(ends)(lambda: line(way, g, d, t, True).wait_recv())

    if straight:
        for t in range(2):
            pl.when(me == n - 1)(lambda: far(t).start())
    start(1, 0)
    for g in range(1, kv_heads):
        start(1, g, (0,))
    loads = []
    for g in range(kv_heads):
        for t, (src, dst) in enumerate(((k_hbm, kall), (v_hbm, vall))):
            load = pltpu.make_async_copy(
                src.at[0, :, pl.ds(g * HEAD, HEAD)], block(dst, g, me), in_sem.at[2 * g + t]
            )
            load.start()
            loads.append(load)
    metas = []
    for src, dst in ((lengths_hbm, lengths), (order_hbm, order), (owner_hbm, owner)):
        metas.append(pltpu.make_async_copy(src, dst, meta_sem.at[len(metas)]))
        metas[-1].start()
    q_load = pltpu.make_async_copy(q_hbm.at[0], q, in_sem.at[2 * kv_heads])
    q_load.start()

    pl.when(me < n - 1)(lambda: pl.semaphore_wait(upper_sem, 1))
    start(0, 0)
    for g in range(1, kv_heads):
        start(0, g, (0,))

    vall[:, :, HEAD:] = jnp.ones((kv_heads, n * tok, HEAD), vall.dtype)
    for meta in metas:
        meta.wait()
    begins = [0]
    for r in range(lengths.shape[1] - 1):
        begins.append(begins[-1] + lengths[0, r])

    def request(position):
        page = position // PAGE
        total = jnp.zeros_like(position)
        for begin in begins[1:]:
            total = total + (page >= begin).astype(jnp.int32)
        return total

    q_pos = order[0, me] * tok + lax.broadcasted_iota(jnp.int32, (tok, 1), 0)
    q_req = request(q_pos)

    def mask(i, _):
        k_pos = order[0, i] * tok + lax.broadcasted_iota(jnp.int32, (1, tok), 1)
        allowed = (request(k_pos) == q_req) & (k_pos <= q_pos)
        bias[:, pl.ds(pl.multiple_of(i * tok, tok), tok)] = jnp.where(allowed, 0.0, NEG)
        return 0

    lax.fori_loop(0, n, mask, 0)

    for d in range(1, n - 1):
        pass_on(0, d)
    for g in range(1, kv_heads):
        for way in range(2):
            start(way, g, (1,))
    for load in loads:
        load.wait()
    q_load.wait()
    pl.when(sec < sections - 1)(lambda: pl.semaphore_wait(next_sem, 1))

    factor = math.log2(math.e) / math.sqrt(HEAD)

    def hand(h):
        cols = pl.ds(pl.multiple_of(h * HEAD, HEAD), HEAD)
        return pltpu.make_async_remote_copy(
            src_ref=ctx.at[:, cols],
            dst_ref=handed.at[:, cols],
            send_sem=hand_send.at[h],
            recv_sem=hand_recv.at[h],
            device_id={"section": onward},
            device_id_type=MESH,
        )

    def weigh(g, h, rows):
        score = lax.dot_general(
            q[rows, pl.ds(h * HEAD, HEAD)],
            kall[g],
            (((1,), (1,)), ((), ())),
            preferred_element_type=jnp.float32,
        )
        score = score * factor + bias[rows, :]
        top = jnp.max(score, axis=1, keepdims=True)
        return jnp.exp2(score - top).astype(jnp.bfloat16)

    def mix(g, h, rows, weight):
        mixed = jnp.dot(weight, vall[g], preferred_element_type=jnp.float32)
        mixed = mixed[:, :HEAD] / mixed[:, HEAD:]
        ctx[rows, pl.ds(h * HEAD, HEAD)] = mixed.astype(ctx.dtype)

    def heads(g, low, high):
        several = range(g * width + low, g * width + high)
        halves = [pl.ds(part * half, half) for part in range(2)]
        if low == 0:
            settle(g, 0)
            for rows in halves:
                for i, h in enumerate(several):
                    weights[i, rows, :] = weigh(g, h, rows)
            settle(g, 1)
            for i, h in enumerate(several):
                for rows in halves:
                    mix(g, h, rows, weights[i, rows, :])
                hand(h).start()
        else:
            for rows in halves:
                for h in several:
                    mix(g, h, rows, weigh(g, h, rows))
            for h in several:
                hand(h).start()

    for g in range(kv_heads):
        last = g + 1 == kv_heads
        for low in range(0, width, 2):
            heads(g, low, min(low + 2, width))
            d = low // 2 + 1
            if not last and d < n - 1 and low + 2 < width:
                pass_on(g + 1, d)
        if not last:
            for d in range((width - 1) // 2 + 1, n - 1):
                pass_on(g + 1, d)

    taken = slots * PAGE
    lane_page = lax.broadcasted_iota(jnp.int32, (1, tok), 1) // PAGE
    lane_token = lax.broadcasted_iota(jnp.int32, (1, tok), 1) % PAGE

    def pick(i, _):
        base = order[0, i] * pages
        target = jnp.full((1, tok), -1, jnp.int32)
        rank = jnp.int32(0)
        for p in range(pages):
            mine = owner[0, base + p] == me
            target = jnp.where(lane_page == p, jnp.where(mine, rank * PAGE, -taken), target)
            rank = rank + mine.astype(jnp.int32)
        target = target + lane_token
        select = (lax.broadcasted_iota(jnp.int32, (taken, tok), 0) == target).astype(jnp.bfloat16)
        rows = pl.ds(pl.multiple_of(i * tok, tok), tok)
        outs = pl.ds(pl.multiple_of(i * taken, taken), taken)
        for g in range(kv_heads):
            cols = pl.ds(g * HEAD, HEAD)
            for dst, src in ((ck, kall), (cv, vall)):
                dst[outs, cols] = jnp.dot(
                    select, src[g, rows, :HEAD], preferred_element_type=jnp.float32
                ).astype(dst.dtype)
        return 0

    lax.fori_loop(0, n, pick, 0)
    for g in range(kv_heads):
        for d in range(1, n):
            for t in range(2):
                for way in range(2):
                    pl.when(sends(way, g, d))(lambda: line(way, g, d, t, False).wait_send())

    if straight:
        for t in range(2):
            pl.when(me == n - 1)(lambda: far(t).wait_send())

    def finish(h, _):
        copy = hand(h)
        copy.wait_send()
        copy.wait_recv()
        return 0

    lax.fori_loop(0, kv_heads * width, finish, 0)


def store(handed_v, ck_v, cv_v, handed, ck, cv, sem):
    copies = []
    for src, dst in ((handed_v, handed), (ck_v, ck), (cv_v, cv)):
        rows = src.shape[0] // 4
        view = dst.at[0] if dst.ndim == 3 else dst.at[0, 0]
        for part in range(4):
            piece = pl.ds(part * rows, rows)
            copies.append(
                pltpu.make_async_copy(src.at[piece], view.at[piece], sem.at[len(copies)])
            )
    for copy in copies:
        copy.start()
    for copy in copies:
        copy.wait()


def body(queries, key_rows, values, lengths, block_order, page_owner):
    n, sections = lax.axis_size("seq"), lax.axis_size("section")
    tok = key_rows.shape[1]
    kv_heads = key_rows.shape[2] // HEAD
    heads = queries.shape[2] // HEAD
    slots = max(2, 2 * (tok // PAGE) // n)
    cores = lax.axis_size("kv")
    dims = (n, sections, cores, tok, kv_heads, heads // kv_heads, slots)
    steps = max(n - 1, 1)
    taken = n * slots * PAGE
    dtype = queries.dtype
    hbm = pl.BlockSpec(memory_space=pltpu.HBM)
    metas = lengths, block_order, page_owner.reshape(page_owner.shape[:2])
    vmem = pl.BlockSpec(memory_space=pltpu.VMEM)
    width = key_rows.shape[2]
    held = pl.pallas_call(
        functools.partial(kernel, dims),
        out_shape=(
            pltpu.VMEM(queries.shape[1:], dtype),
            pltpu.VMEM((taken, width), dtype),
            pltpu.VMEM((taken, width), dtype),
        ),
        in_specs=[hbm] * 6,
        out_specs=(vmem, vmem, vmem),
        scratch_shapes=[
            pltpu.VMEM((tok, heads * HEAD), dtype),
            pltpu.VMEM((kv_heads, n * tok, HEAD), dtype),
            pltpu.VMEM((kv_heads, n * tok, 2 * HEAD), dtype),
            pltpu.VMEM((tok, n * tok), jnp.float32),
            pltpu.VMEM((2, tok, n * tok), dtype),
            pltpu.VMEM((tok, heads * HEAD), dtype),
            *(pltpu.SMEM(x.shape, x.dtype) for x in metas),
            pltpu.SemaphoreType.DMA((3,)),
            pltpu.SemaphoreType.DMA((2 * kv_heads + 1,)),
            pltpu.SemaphoreType.DMA((2, kv_heads, steps, 2)),
            pltpu.SemaphoreType.DMA((2, kv_heads, steps, 2)),
            pltpu.SemaphoreType.DMA((2,)),
            pltpu.SemaphoreType.REGULAR,
            pltpu.SemaphoreType.REGULAR,
            pltpu.SemaphoreType.DMA((heads,)),
            pltpu.SemaphoreType.DMA((heads,)),
        ],
        compiler_params=pltpu.CompilerParams(
            collective_id=0, has_side_effects=True, vmem_limit_bytes=48 << 20
        ),
    )(
        *(
            pltpu.with_memory_space_constraint(x, pltpu.HBM)
            for x in (*metas, queries, key_rows, values)
        ),
    )
    return pl.pallas_call(
        store,
        out_shape=(
            jax.ShapeDtypeStruct(queries.shape, dtype),
            jax.ShapeDtypeStruct((1, 1, taken, width), dtype),
            jax.ShapeDtypeStruct((1, 1, taken, width), dtype),
        ),
        in_specs=[vmem, vmem, vmem],
        out_specs=(hbm, hbm, hbm),
        scratch_shapes=[pltpu.SemaphoreType.DMA((12,))],
        compiler_params=pltpu.CompilerParams(vmem_limit_bytes=8 << 20),
    )(*(pltpu.with_memory_space_constraint(x, pltpu.VMEM) for x in held))


def solution(mesh):
    in_specs = (
        P(("groups", "section"), "seq", "kv"),
        P(("groups", "section"), "seq", "kv"),
        P(("groups", "section"), "seq", "kv"),
        P(("groups", "section"), None),
        P(("groups", "section"), None),
        P(("groups", "section"), None, None),
    )
    out_specs = (
        P(("groups", "section"), "seq", "kv"),
        P(("groups", "section"), "seq", None, "kv"),
        P(("groups", "section"), "seq", None, "kv"),
    )
    return jax.shard_map(body, mesh=mesh, in_specs=in_specs, out_specs=out_specs, check_vma=False)
```

```python
import functools
import math

import jax
import jax.numpy as jnp
from jax import lax
from jax.experimental import pallas as pl
from jax.experimental.pallas import tpu as pltpu
from jax.sharding import PartitionSpec as P

HEAD = 128
PAGE = 16
NEG = -1e30
MESH = pl.DeviceIdType.MESH


def greet(barrier, peer):
    pl.semaphore_signal(barrier, inc=1, device_id=peer, device_id_type=MESH)


def kernel(
    dims,
    lengths_hbm,
    order_hbm,
    owner_hbm,
    q_hbm,
    k_hbm,
    v_hbm,
    handed,
    ck,
    cv,
    q,
    kall,
    vall,
    bias,
    weights,
    ctx,
    lengths,
    order,
    owner,
    meta_sem,
    in_sem,
    send_sem,
    recv_sem,
    far_send,
    upper_sem,
    next_sem,
    hand_send,
    hand_recv,
):
    n, sections, cores, tok, kv_heads, width, slots = dims
    pages = tok // PAGE
    me = lax.axis_index("seq")
    sec = lax.axis_index("section")
    core = lax.axis_index("kv")
    right, left = me + 1, me - 1
    onward = lax.rem(sec + 1, sections)
    straight = n > 2
    half = tok // 2

    def block(ref, g, index):
        rows = pl.ds(pl.multiple_of(index * tok, tok), tok)
        return ref.at[g, rows, pl.ds(0, HEAD)]

    barrier = pltpu.get_barrier_semaphore()
    below = jnp.where(me > 0, 1, 0) + jnp.where(sec > 0, 1, 0)
    pl.when(below > 0)(lambda: pl.semaphore_wait(barrier, below))
    pl.when(me < n - 1)(lambda: greet(barrier, {"seq": right}))
    pl.when(sec < sections - 1)(lambda: greet(barrier, {"section": sec + 1}))
    pl.when(me > 0)(lambda: greet(upper_sem, {"seq": left}))
    pl.when(sec > 0)(lambda: greet(next_sem, {"section": sec - 1}))

    def sends(way, g, d):
        if way == 0:
            return (me < n - 1) & (me >= d - 1)
        if straight and g == 0 and d == n - 1:
            return me < 0
        return (me > 0) & (me <= n - d)

    def takes(way, d):
        return me >= d if way == 0 else me + d <= n - 1

    def line(way, g, d, t, arriving):
        shift = d if arriving else d - 1
        ref = block((kall, vall)[t], g, me - shift if way == 0 else me + shift)
        src = ref
        if d == 1 and not arriving:
            src = (k_hbm, v_hbm)[t].at[0, :, pl.ds(g * HEAD, HEAD)]
        return pltpu.make_async_remote_copy(
            src_ref=src,
            dst_ref=ref,
            send_sem=send_sem.at[way, g, d - 1, t],
            recv_sem=recv_sem.at[way, g, d - 1, t],
            device_id={"seq": right if way == 0 else left},
            device_id_type=MESH,
        )

    def far(t):
        return pltpu.make_async_remote_copy(
            src_ref=(k_hbm, v_hbm)[t].at[0, :, pl.ds(0, HEAD)],
            dst_ref=block((kall, vall)[t], 0, me),
            send_sem=far_send.at[t],
            recv_sem=recv_sem.at[1, 0, n - 2, t],
            device_id={"seq": 0},
            device_id_type=MESH,
        )

    def start(way, g, ts=(0, 1)):
        for t in ts:
            pl.when(sends(way, g, 1))(lambda: line(way, g, 1, t, False).start())

    def pass_on(g, d):
        for t in range(2):
            for way in range(2):

                @pl.when(sends(way, g, d + 1))
                def _():
                    line(way, g, d, t, True).wait_recv()
                    line(way, g, d + 1, t, False).start()

    def settle(g, t):
        for d in range(1, n):
            for way in range(2):
                ends = takes(way, d) & jnp.logical_not(sends(way, g, d + 1))
                pl.when(ends)(lambda: line(way, g, d, t, True).wait_recv())

    for t in range(2):
        if straight:
            pl.when(me == n - 1)(lambda: far(t).start())
        start(1, 0, (t,))
    for g in range(1, kv_heads):
        start(1, g, (0,))
    loads = []
    for g in range(kv_heads):
        for t, (src, dst) in enumerate(((k_hbm, kall), (v_hbm, vall))):
            load = pltpu.make_async_copy(
                src.at[0, :, pl.ds(g * HEAD, HEAD)], block(dst, g, me), in_sem.at[2 * g + t]
            )
            load.start()
            loads.append(load)
    metas = []
    for src, dst in ((lengths_hbm, lengths), (order_hbm, order), (owner_hbm, owner)):
        metas.append(pltpu.make_async_copy(src, dst, meta_sem.at[len(metas)]))
        metas[-1].start()
    q_load = pltpu.make_async_copy(q_hbm.at[0], q, in_sem.at[2 * kv_heads])
    q_load.start()

    pl.when(me < n - 1)(lambda: pl.semaphore_wait(upper_sem, 1))
    start(0, 0)
    for g in range(1, kv_heads):
        start(0, g, (0,))

    vall[:, :, HEAD:] = jnp.ones((kv_heads, n * tok, HEAD), vall.dtype)
    for meta in metas:
        meta.wait()
    begins = [0]
    for r in range(lengths.shape[1] - 1):
        begins.append(begins[-1] + lengths[0, r])

    def request(position):
        page = position // PAGE
        total = jnp.zeros_like(position)
        for begin in begins[1:]:
            total = total + (page >= begin).astype(jnp.int32)
        return total

    q_pos = order[0, me] * tok + lax.broadcasted_iota(jnp.int32, (tok, 1), 0)
    q_req = request(q_pos)

    def mask(i, _):
        k_pos = order[0, i] * tok + lax.broadcasted_iota(jnp.int32, (1, tok), 1)
        allowed = (request(k_pos) == q_req) & (k_pos <= q_pos)
        bias[:, pl.ds(pl.multiple_of(i * tok, tok), tok)] = jnp.where(allowed, 0.0, NEG)
        return 0

    lax.fori_loop(0, n, mask, 0)

    for d in range(1, n - 1):
        pass_on(0, d)
    for g in range(1, kv_heads):
        for way in range(2):
            start(way, g, (1,))
    for load in loads:
        load.wait()
    q_load.wait()
    pl.when(sec < sections - 1)(lambda: pl.semaphore_wait(next_sem, 1))

    factor = math.log2(math.e) / math.sqrt(HEAD)

    def hand(h):
        cols = pl.ds(pl.multiple_of(h * HEAD, HEAD), HEAD)
        return pltpu.make_async_remote_copy(
            src_ref=ctx.at[:, cols],
            dst_ref=handed.at[:, cols],
            send_sem=hand_send.at[h],
            recv_sem=hand_recv.at[h],
            device_id={"section": onward},
            device_id_type=MESH,
        )

    def weigh(g, h, rows):
        score = lax.dot_general(
            q[rows, pl.ds(h * HEAD, HEAD)],
            kall[g],
            (((1,), (1,)), ((), ())),
            preferred_element_type=jnp.float32,
        )
        score = score * factor + bias[rows, :]
        top = jnp.max(score, axis=1, keepdims=True)
        return jnp.exp2(score - top).astype(jnp.bfloat16)

    def mix(g, h, rows, weight):
        mixed = jnp.dot(weight, vall[g], preferred_element_type=jnp.float32)
        mixed = mixed[:, :HEAD] / mixed[:, HEAD:]
        ctx[rows, pl.ds(h * HEAD, HEAD)] = mixed.astype(ctx.dtype)

    def heads(g, low, high):
        several = range(g * width + low, g * width + high)
        halves = [pl.ds(part * half, half) for part in range(2)]
        if low == 0:
            settle(g, 0)
            for rows in halves:
                for i, h in enumerate(several):
                    weights[i, rows, :] = weigh(g, h, rows)
            settle(g, 1)
            for i, h in enumerate(several):
                for rows in halves:
                    mix(g, h, rows, weights[i, rows, :])
                hand(h).start()
        else:
            for rows in halves:
                for h in several:
                    mix(g, h, rows, weigh(g, h, rows))
            for h in several:
                hand(h).start()

    for g in range(kv_heads):
        last = g + 1 == kv_heads
        for low in range(0, width, 2):
            heads(g, low, min(low + 2, width))
            d = low // 2 + 1
            if not last and d < n - 1 and low + 2 < width:
                pass_on(g + 1, d)
        if not last:
            for d in range((width - 1) // 2 + 1, n - 1):
                pass_on(g + 1, d)

    taken = slots * PAGE
    lane_page = lax.broadcasted_iota(jnp.int32, (1, tok), 1) // PAGE
    lane_token = lax.broadcasted_iota(jnp.int32, (1, tok), 1) % PAGE

    def pick(i, _):
        base = order[0, i] * pages
        target = jnp.full((1, tok), -1, jnp.int32)
        rank = jnp.int32(0)
        for p in range(pages):
            mine = owner[0, base + p] == me
            target = jnp.where(lane_page == p, jnp.where(mine, rank * PAGE, -taken), target)
            rank = rank + mine.astype(jnp.int32)
        target = target + lane_token
        select = (lax.broadcasted_iota(jnp.int32, (taken, tok), 0) == target).astype(jnp.bfloat16)
        rows = pl.ds(pl.multiple_of(i * tok, tok), tok)
        outs = pl.ds(pl.multiple_of(i * taken, taken), taken)
        for g in range(kv_heads):
            cols = pl.ds(g * HEAD, HEAD)
            for dst, src in ((ck, kall), (cv, vall)):
                dst[outs, cols] = jnp.dot(
                    select, src[g, rows, :HEAD], preferred_element_type=jnp.float32
                ).astype(dst.dtype)
        return 0

    lax.fori_loop(0, n, pick, 0)
    for g in range(kv_heads):
        for d in range(1, n):
            for t in range(2):
                for way in range(2):
                    pl.when(sends(way, g, d))(lambda: line(way, g, d, t, False).wait_send())

    if straight:
        for t in range(2):
            pl.when(me == n - 1)(lambda: far(t).wait_send())

    def finish(h, _):
        copy = hand(h)
        copy.wait_send()
        copy.wait_recv()
        return 0

    lax.fori_loop(0, kv_heads * width, finish, 0)


def store(handed_v, ck_v, cv_v, handed, ck, cv, sem):
    copies = []
    for src, dst in ((handed_v, handed), (ck_v, ck), (cv_v, cv)):
        rows = src.shape[0] // 4
        view = dst.at[0] if dst.ndim == 3 else dst.at[0, 0]
        for part in range(4):
            piece = pl.ds(part * rows, rows)
            copies.append(
                pltpu.make_async_copy(src.at[piece], view.at[piece], sem.at[len(copies)])
            )
    for copy in copies:
        copy.start()
    for copy in copies:
        copy.wait()


def body(queries, key_rows, values, lengths, block_order, page_owner):
    n, sections = lax.axis_size("seq"), lax.axis_size("section")
    tok = key_rows.shape[1]
    kv_heads = key_rows.shape[2] // HEAD
    heads = queries.shape[2] // HEAD
    slots = max(2, 2 * (tok // PAGE) // n)
    cores = lax.axis_size("kv")
    dims = (n, sections, cores, tok, kv_heads, heads // kv_heads, slots)
    steps = max(n - 1, 1)
    taken = n * slots * PAGE
    dtype = queries.dtype
    hbm = pl.BlockSpec(memory_space=pltpu.HBM)
    metas = lengths, block_order, page_owner.reshape(page_owner.shape[:2])
    vmem = pl.BlockSpec(memory_space=pltpu.VMEM)
    width = key_rows.shape[2]
    held = pl.pallas_call(
        functools.partial(kernel, dims),
        out_shape=(
            pltpu.VMEM(queries.shape[1:], dtype),
            pltpu.VMEM((taken, width), dtype),
            pltpu.VMEM((taken, width), dtype),
        ),
        in_specs=[hbm] * 6,
        out_specs=(vmem, vmem, vmem),
        scratch_shapes=[
            pltpu.VMEM((tok, heads * HEAD), dtype),
            pltpu.VMEM((kv_heads, n * tok, HEAD), dtype),
            pltpu.VMEM((kv_heads, n * tok, 2 * HEAD), dtype),
            pltpu.VMEM((tok, n * tok), jnp.float32),
            pltpu.VMEM((2, tok, n * tok), dtype),
            pltpu.VMEM((tok, heads * HEAD), dtype),
            *(pltpu.SMEM(x.shape, x.dtype) for x in metas),
            pltpu.SemaphoreType.DMA((3,)),
            pltpu.SemaphoreType.DMA((2 * kv_heads + 1,)),
            pltpu.SemaphoreType.DMA((2, kv_heads, steps, 2)),
            pltpu.SemaphoreType.DMA((2, kv_heads, steps, 2)),
            pltpu.SemaphoreType.DMA((2,)),
            pltpu.SemaphoreType.REGULAR,
            pltpu.SemaphoreType.REGULAR,
            pltpu.SemaphoreType.DMA((heads,)),
            pltpu.SemaphoreType.DMA((heads,)),
        ],
        compiler_params=pltpu.CompilerParams(
            collective_id=0, has_side_effects=True, vmem_limit_bytes=48 << 20
        ),
    )(
        *(
            pltpu.with_memory_space_constraint(x, pltpu.HBM)
            for x in (*metas, queries, key_rows, values)
        ),
    )
    return pl.pallas_call(
        store,
        out_shape=(
            jax.ShapeDtypeStruct(queries.shape, dtype),
            jax.ShapeDtypeStruct((1, 1, taken, width), dtype),
            jax.ShapeDtypeStruct((1, 1, taken, width), dtype),
        ),
        in_specs=[vmem, vmem, vmem],
        out_specs=(hbm, hbm, hbm),
        scratch_shapes=[pltpu.SemaphoreType.DMA((12,))],
        compiler_params=pltpu.CompilerParams(vmem_limit_bytes=8 << 20),
    )(*(pltpu.with_memory_space_constraint(x, pltpu.VMEM) for x in held))


def solution(mesh):
    in_specs = (
        P(("groups", "section"), "seq", "kv"),
        P(("groups", "section"), "seq", "kv"),
        P(("groups", "section"), "seq", "kv"),
        P(("groups", "section"), None),
        P(("groups", "section"), None),
        P(("groups", "section"), None, None),
    )
    out_specs = (
        P(("groups", "section"), "seq", "kv"),
        P(("groups", "section"), "seq", None, "kv"),
        P(("groups", "section"), "seq", None, "kv"),
    )
    return jax.shard_map(body, mesh=mesh, in_specs=in_specs, out_specs=out_specs, check_vma=False)
```
